32 devices in a mesh: rows: 8 (over z, x), heads: 4 (over y, core).
Axes of the slice: x: 2, y: 2, z: 4, core: 2. Of those that a mesh axis runs over, the one named last changes fastest.
Arguments:
- pair_tensor: bfloat16 [192, 192, 128], P('rows'), may hold values from -8 to 8
- lengths: int32 [1], replicated, may hold values from 96 to 192
- starting_gain: float32 [128], replicated, may hold values from 0.25 to 1.75
- starting_weights: bfloat16 [128, 512], P(None, 'heads'), may hold values from -1 to 1
- starting_bias: bfloat16 [4, 128], P('heads'), may hold values from -12 to 12
- starting_output: bfloat16 [128, 128], replicated, may hold values from -0.5 to 0.5
- ending_gain: float32 [128], replicated, may hold values from 0.25 to 1.75
- ending_weights: bfloat16 [128, 512], P(None, 'heads'), may hold values from -1 to 1
- ending_bias: bfloat16 [4, 128], P('heads'), may hold values from -12 to 12
- ending_output: bfloat16 [128, 128], replicated, may hold values from -0.5 to 0.5
Outputs:
- refined: bfloat16 [192, 192, 128], P(('rows', 'heads'))
The draws below stay inside these ranges and needn't reach their ends.
All inputs are finite; a program needn't handle non-finite values.
Results may differ from the reference program's by a relative error of at most 0.009.
The reference program's roundings to bfloat16 on the way count: a program that leaves them out, or rounds other values in their place, can miss the bound.
Values may be sent and summed in bfloat16 or wider, within the bound.
No kernel may reach another device: no remote copies, remote signals or barrier semaphores. Data moves between devices by JAX's collectives and lax.ppermute only.
A program may use at most 128 MiB of HBM per device.

```python
import jax
import jax.numpy as jnp
from jax import lax

C = 128
H = 4
DH = 32
N = 192


def draw_pair_tensor(key, part):
    first_key = jax.random.fold_in(key, 11)
    value_key = jax.random.fold_in(first_key, 0)
    values = jax.random.normal(value_key, (N, N, C), jnp.float32)
    return jnp.clip(values, -8.0, 8.0).astype(jnp.bfloat16)


def draw_starting_bias(key, part):
    noise_rows = jax.random.normal(jax.random.fold_in(key, 21), (H, C), jnp.float32) * (1.5 / jnp.sqrt(jnp.float32(C)))
    values = noise_rows
    return jnp.clip(values, -12.0, 12.0).astype(jnp.bfloat16)


def draw_ending_bias(key, part):
    noise_rows = jax.random.normal(jax.random.fold_in(key, 22), (H, C), jnp.float32) * (1.5 / jnp.sqrt(jnp.float32(C)))
    values = noise_rows
    return jnp.clip(values, -12.0, 12.0).astype(jnp.bfloat16)


def shard_levels(rng, shape, cuts, smallest, largest):
    loudness, own = 1.0, jax.random.fold_in(rng, 6)
    for axis_at, parts in cuts:
        steps = jnp.exp(jax.random.uniform(jax.random.fold_in(own, axis_at), (parts,), jnp.float32, smallest / len(cuts), largest / len(cuts)))
        loudness = loudness * jnp.repeat(steps, shape[axis_at] // parts).reshape([-1 if axis == axis_at else 1 for axis in range(len(shape))])
    return loudness


def normal_values(own_key, dims, deviation, bound, cuts=(), kind=jnp.bfloat16):
    values = jax.random.normal(own_key, dims, jnp.float32) * deviation
    if len(cuts) > 0:
        values = shard_levels(own_key, dims, cuts, -0.22, 0.18) * values
    return jnp.clip(values, min=-bound, max=bound).astype(kind)


def setup_inputs(seed: int = 0) -> dict:
    arg_keys = jax.random.split(jax.random.key(seed), 11)
    pair_tensor = draw_pair_tensor(jax.random.fold_in(arg_keys[10], 71), 0)
    lengths = jax.random.randint(arg_keys[1], (1,), N // 2, N + 1).astype(jnp.int32)
    starting_gain = jnp.clip(1.0 + 0.15 * jax.random.normal(arg_keys[2], (C,), jnp.float32), 0.25, 1.75)
    starting_weights = normal_values(arg_keys[3], (C, H * 4 * DH), (C // 3) ** -0.5, 1.0, ((1, 4),))
    starting_bias = draw_starting_bias(jax.random.fold_in(arg_keys[10], 71), 0)
    starting_output = normal_values(arg_keys[5], (H * DH, C), (H * DH) ** -0.5, 0.5)
    ending_gain = jnp.clip(1.0 + 0.15 * jax.random.normal(arg_keys[6], (C,), jnp.float32), 0.25, 1.75)
    ending_weights = normal_values(arg_keys[7], (C, H * 4 * DH), (C // 3) ** -0.5, 1.0, ((1, 4),))
    ending_bias = draw_ending_bias(jax.random.fold_in(arg_keys[10], 71), 0)
    ending_output = normal_values(arg_keys[9], (H * DH, C), (H * DH) ** -0.5, 0.5)
    return {"pair_tensor": pair_tensor, "lengths": lengths, "starting_gain": starting_gain, "starting_weights": starting_weights, "starting_bias": starting_bias, "starting_output": starting_output, "ending_gain": ending_gain, "ending_weights": ending_weights, "ending_bias": ending_bias, "ending_output": ending_output}


epsilon = 1e-05
masked_score = -1000000000.0

def layer_normed(values, scales):
    widened = values.astype(jnp.float32)
    centre = lax.optimization_barrier(jnp.mean(widened, axis=-1, keepdims=True))
    shifted = widened - centre
    spread = lax.optimization_barrier(jnp.mean(shifted * shifted, axis=-1, keepdims=True))
    return (shifted * lax.rsqrt(spread + epsilon) * scales).astype(jnp.bfloat16)

def node_update(tensor, scales, weights, bias_rows, output_rows, lengths):
    normed = layer_normed(tensor, scales)
    head_count = bias_rows.shape[0]
    channels = tensor.shape[2]
    head_width = weights.shape[1] // (4 * head_count)
    key_count = tensor.shape[1]
    bias_plane = jnp.einsum('abc,hc->hab', normed.astype(jnp.float32), bias_rows.astype(jnp.float32))
    allowed = jnp.arange(key_count) < lengths[0]
    factor = 1.0 / jnp.sqrt(jnp.float32(head_width))
    shaped_weights = weights.astype(jnp.float32).reshape(channels, head_count, 4, head_width)
    out_weights = output_rows.astype(jnp.float32).reshape(head_count, head_width, channels)

    def block_rows(normed_block):
        projected = jnp.einsum('abc,chkd->abhkd', normed_block.astype(jnp.float32), shaped_weights)
        queries = projected[:, :, :, 0].astype(jnp.bfloat16)
        keys_part = projected[:, :, :, 1].astype(jnp.bfloat16)
        values_part = projected[:, :, :, 2].astype(jnp.bfloat16)
        gate_values = jax.nn.sigmoid(projected[:, :, :, 3])
        scores = jnp.einsum('abhd,akhd->ahbk', queries.astype(jnp.float32), keys_part.astype(jnp.float32)) * factor + bias_plane[None]
        scores = jnp.where(allowed, scores, masked_score)
        highest = lax.optimization_barrier(jnp.max(scores, axis=-1, keepdims=True))
        raised = jnp.exp(scores - highest)
        weights_low = (raised / lax.optimization_barrier(jnp.sum(raised, axis=-1, keepdims=True))).astype(jnp.bfloat16)
        attended = jnp.einsum('ahbk,akhd->abhd', weights_low.astype(jnp.float32), values_part.astype(jnp.float32))
        gated_out = (gate_values * attended).astype(jnp.bfloat16)
        return jnp.einsum('abhd,hdc->abc', gated_out.astype(jnp.float32), out_weights)
    row_count = tensor.shape[0]
    blocks = normed.reshape(row_count // 8, 8, key_count, channels)
    return lax.map(block_rows, blocks).reshape(row_count, key_count, channels)

def reference(pair_tensor, lengths, starting_gain, starting_weights, starting_bias, starting_output, ending_gain, ending_weights, ending_bias, ending_output):
    update_first = node_update(pair_tensor, starting_gain, starting_weights, starting_bias, starting_output, lengths)
    middle = (pair_tensor.astype(jnp.float32) + update_first).astype(jnp.bfloat16)
    update_turned = node_update(jnp.swapaxes(middle, 0, 1), ending_gain, ending_weights, ending_bias, ending_output, lengths)
    update_second = jnp.swapaxes(update_turned, 0, 1).astype(jnp.bfloat16)
    return (middle.astype(jnp.float32) + update_second.astype(jnp.float32)).astype(jnp.bfloat16)
```

```python
import functools
import math

import jax
import jax.numpy as jnp
from jax import lax
from jax.experimental import pallas as pl
from jax.experimental.pallas import tpu as pltpu
from jax.sharding import PartitionSpec as P

epsilon = 1e-05
masked_score = -1e30
log2e = math.log2(math.e)
steps = 32767.0
f32 = jnp.float32
bf16 = jnp.bfloat16
both = ("rows", "heads")


def up(value, multiple):
    return -(-value // multiple) * multiple


class Sizes:
    def __init__(self, tokens, channels, row_devices, heads):
        self.N, self.C, self.R, self.H = tokens, channels, row_devices, heads
        self.D = row_devices * heads
        self.L = tokens // row_devices
        self.T = tokens // self.D
        self.NP = up(tokens, 128)
        self.full = tokens // 128
        self.rest = tokens % 128
        self.pair = self.rest == 64
        groups = self.L // 8
        self.c1 = self.L * self.full
        if self.rest:
            self.c1 += 8 * (-(-groups // 2) if self.pair else groups)
        self.p2 = self.T * heads * self.full
        if self.rest:
            self.p2 += self.T * (heads // 2 if self.pair else heads)
        self.c2 = up(self.p2 + self.T * self.T, 8)
        self.c3 = up(self.T * self.T, 8)
        self.JB = tokens if tokens <= 256 else 192
        self.W = channels // heads


def each(count, body):
    if count == 1:
        body(0)
    else:

        @pl.loop(0, count)
        def _(index):
            body(index)


def at(index, size):
    if isinstance(index, int):
        return pl.ds(index * size, size)
    return pl.ds(pl.multiple_of(index * size, 8), size)


def nt(left, right):
    return lax.dot_general(left, right, (((1,), (1,)), ((), ())), preferred_element_type=f32)


def normalise(widened, gain):
    centre = jnp.mean(widened, axis=-1, keepdims=True)
    shifted = widened - centre
    spread = jnp.mean(shifted * shifted, axis=-1, keepdims=True)
    return (shifted * lax.rsqrt(spread + epsilon) * gain).astype(bf16)


def plane_bound(gain, bias, channels):
    product = gain * bias
    norm = jnp.sqrt(jnp.sum(product * product, axis=-1, keepdims=True))
    return jnp.maximum(norm * (1.01 * math.sqrt(channels)), 1e-20)


def normed_bound(gain, channels):
    return jnp.max(jnp.abs(gain), axis=-1, keepdims=True) * (1.01 * math.sqrt(channels))


def coded(values):
    return jnp.round(values).astype(jnp.int32).astype(jnp.int16)


def decoded(values):
    return values.astype(jnp.int32).astype(f32)


def first_plane_kernel(z, pair_ref, gain_ref, bias_ref, w1_ref, w2_ref, b2_ref, out_ref, weights_ref, plane_ref, pack_ref):
    C, L = z.C, z.L
    gain = gain_ref[...]
    bias = bias_ref[...]
    weights_ref[0:C] = w1_ref[...]
    weights_ref[C : 2 * C] = w2_ref[...]
    row = lax.broadcasted_iota(jnp.int32, (16, C), 0)
    weights_ref[2 * C : 2 * C + 16] = jnp.where(row == 0, bias.astype(f32), b2_ref[...].astype(f32)).astype(bf16)
    factor = steps / plane_bound(gain, bias.astype(f32), C)
    many = jnp.broadcast_to(bias.astype(f32), (8, C)).astype(bf16)
    sub = lax.broadcasted_iota(jnp.int32, (8, z.N), 0)

    @pl.loop(0, L // 8)
    def _(group):
        tile = jnp.zeros((8, z.N), f32)
        for j in range(8):
            normed = normalise(pair_ref[group * 8 + j].astype(f32), gain)
            tile = jnp.where(sub == j, nt(many, normed), tile)
        plane_ref[at(group, 8), 0 : z.N] = tile * factor

    for tile in range(z.full):
        pack_ref[tile * L : (tile + 1) * L] = plane_ref[:, tile * 128 : (tile + 1) * 128]
    base = z.full * L
    if z.rest:
        last = plane_ref[:, z.full * 128 : z.full * 128 + 128]
        lane = lax.broadcasted_iota(jnp.int32, (8, 128), 1)
        groups = L // 8
        step = 2 if z.pair else 1
        for slot, group in enumerate(range(0, groups, step)):
            value = last[group * 8 : group * 8 + 8]
            if z.pair and group + 1 < groups:
                other = pltpu.roll(last[group * 8 + 8 : group * 8 + 16], 64, 1)
                value = jnp.where(lane < 64, value, other)
            else:
                value = jnp.where(lane < z.rest, value, 0.0)
            pack_ref[base + slot * 8 : base + slot * 8 + 8] = value
    whole = pack_ref[...]
    twice = coded(jnp.concatenate([whole, whole], axis=0))

    @pl.loop(0, z.D // 2)
    def _(device):
        out_ref[at(device, 2 * z.c1)] = twice


def project(normed, weights):
    C = normed.shape[1]
    projected = jnp.dot(normed, weights, preferred_element_type=f32)
    queries, keys, values = (projected[:, n * C : (n + 1) * C].astype(bf16) for n in range(3))
    gates = 1.0 / (1.0 + jnp.exp(-projected[:, 3 * C :]))
    return queries, keys, values, gates


def project_kernel(z, pair_ref, gain_ref, w_ref, q_ref, k_ref, v_ref, g_ref):
    @pl.loop(0, z.T)
    def _(t):
        def block(b):
            normed = normalise(pair_ref[t, at(b, z.JB)].astype(f32), gain_ref[...])
            q_ref[t, at(b, z.JB)], k_ref[t, at(b, z.JB)], v_ref[t, at(b, z.JB)], g_ref[t, at(b, z.JB)] = project(normed, w_ref[...])

        each(z.N // z.JB, block)
        if z.NP > z.N:
            k_ref[t, z.N :] = jnp.zeros((z.NP - z.N, z.C), bf16)
            v_ref[t, z.N :] = jnp.zeros((z.NP - z.N, z.C), bf16)


def head_masks(z):
    lane = lax.broadcasted_iota(jnp.int32, (1, z.C), 1)
    return [jnp.where((lane >= h * z.W) & (lane < (h + 1) * z.W), 1.0, 0.0).astype(bf16) for h in range(z.H)]


def attended(z, queries, keys, values, planes):
    masks = head_masks(z)
    rows = queries.shape[0]
    stacked = jnp.concatenate([queries * mask for mask in masks], axis=0)
    scores = nt(stacked, keys) * (log2e / math.sqrt(z.W))
    parts = []
    for h in range(z.H):
        score = scores[h * rows : (h + 1) * rows] + planes[h]
        raised = jnp.exp2(score - jnp.max(score, axis=-1, keepdims=True))
        parts.append((raised * (1.0 / jnp.sum(raised, axis=-1, keepdims=True))).astype(bf16))
    return jnp.dot(
        jnp.concatenate(parts, axis=1),
        jnp.concatenate([values * mask for mask in masks], axis=0),
        preferred_element_type=f32,
    )


def first_node_kernel(
    z, lengths_ref, recv_ref, q_ref, k_ref, v_ref, g_ref, pair_ref, gain1_ref, bias1_ref, out_w_ref, gain2_ref, bias2_ref,
    middle_ref, send_ref, raw_ref, plane_ref, row_ref, turned_ref, pay_ref, own_ref,
):
    N, T, H, D, L, C = z.N, z.T, z.H, z.D, z.L, z.C
    length = lengths_ref[0]
    bound1 = plane_bound(gain1_ref[...], bias1_ref[...].astype(f32), C) * (log2e / steps)
    gain2 = gain2_ref[...]
    bias2 = jnp.concatenate([bias2_ref[...].astype(f32), jnp.zeros((8 - H, C), f32)], axis=0)
    factor2 = steps / plane_bound(gain2, bias2, C)
    bias2 = bias2.astype(bf16)
    factor_n = steps / normed_bound(gain2, C)
    lane = lax.broadcasted_iota(jnp.int32, (8, 128), 1)

    @pl.loop(0, D // 2)
    def _(device):
        raw_ref[at(device, 2 * z.c1)] = decoded(recv_ref[at(device, 2 * z.c1)])

    @pl.loop(0, z.R)
    def _(r):
        for h in range(H):
            start = pl.multiple_of((r * H + h) * z.c1, 8)
            scale = bound1[h : h + 1, 0:1]
            target = pl.ds(pl.multiple_of(r * L, 8), L)
            for tile in range(z.full):
                value = raw_ref[pl.ds(start + tile * L, L)] * scale
                seen = lax.broadcasted_iota(jnp.int32, (L, 128), 1) + tile * 128 < length
                plane_ref[h, target, tile * 128 : (tile + 1) * 128] = jnp.where(seen, value, masked_score)
            if z.rest:
                seen = (lane + z.full * 128 < length) & (lane < z.rest)
                for group in range(L // 8):
                    slot = group // 2 if z.pair else group
                    value = raw_ref[pl.ds(start + z.full * L + slot * 8, 8)]
                    if z.pair and group % 2:
                        value = pltpu.roll(value, 64, 1)
                    plane_ref[h, pl.ds(pl.multiple_of(r * L, 8) + group * 8, 8), z.full * 128 :] = jnp.where(seen, value * scale, masked_score)

    @pl.loop(0, T)
    def _(t):
        def block(b):
            span = at(b, z.JB)
            mixed = attended(z, q_ref[t, span], k_ref[t], v_ref[t], [plane_ref[h, span] for h in range(H)])
            gated = (g_ref[t, span] * mixed).astype(bf16)
            update = jnp.dot(gated, out_w_ref[...], preferred_element_type=f32)
            middle = (pair_ref[t, span].astype(f32) + update).astype(bf16)
            middle_ref[t, span] = middle
            row_ref[span] = normalise(middle.astype(f32), gain2).astype(f32)

        each(N // z.JB, block)
        for c in range(T):
            piece = row_ref[pl.ds(c, D, stride=T)]
            turned_ref[c * D : (c + 1) * D] = piece
            pay_ref[pl.ds(z.p2 + t * T + c, D, stride=z.c2)] = jnp.round(piece * factor_n)
        values = nt(bias2, turned_ref[...].astype(bf16)) * factor2
        for tile in range(z.full):
            own_ref[pl.ds((tile * T + t) * H, H)] = values[0:H, tile * 128 : (tile + 1) * 128]
        if z.rest:
            last = jnp.concatenate([values[:, z.full * 128 :], jnp.zeros((8, 128 - z.rest), f32)], axis=1)
            if z.pair:
                other = pltpu.roll(pltpu.roll(last, 64, 1), 8 - H // 2, 0)
                joined = jnp.where(lane < 64, last, other)
                own_ref[pl.ds(z.full * T * H + t * (H // 2), H // 2)] = joined[0 : H // 2]
            else:
                own_ref[pl.ds(z.full * T * H + t * H, H)] = last[0:H]

    own = own_ref[0 : z.p2]

    @pl.loop(0, D)
    def _(device):
        pay_ref[pl.ds(pl.multiple_of(device * z.c2, 8), z.p2)] = own

    @pl.loop(0, D // 2)
    def _(device):
        send_ref[at(device, 2 * z.c2)] = coded(pay_ref[at(device, 2 * z.c2)])


def second_node_kernel(
    z, lengths_ref, recv_ref, w_ref, gain2_ref, bias2_ref, out_w_ref,
    send_ref, raw_ref, column_ref, k_ref, v_ref, q_ref, g_ref, keyed_ref, plane_ref, pay_ref,
):
    N, T, H, D, C = z.N, z.T, z.H, z.D, z.C
    length = lengths_ref[0]
    gain2 = gain2_ref[...]
    bound2 = plane_bound(gain2, bias2_ref[...].astype(f32), C) * (log2e / steps)
    scale_n = normed_bound(gain2, C) * (1.0 / steps)

    @pl.loop(0, D // 2)
    def _(device):
        raw_ref[at(device, 2 * z.c2)] = decoded(recv_ref[at(device, 2 * z.c2)])

    def seen(base):
        slot = lax.broadcasted_iota(jnp.int32, (128, 128), 1) + base
        return ((slot % D) * T + slot // D < length) & (slot < N)

    for h in range(H):
        for t in range(T):
            span = pl.ds(t * D, D)
            for tile in range(z.full):
                keyed_ref[span, tile * 128 : (tile + 1) * 128] = raw_ref[pl.ds((tile * T + t) * H + h, D, stride=z.c2)]
            if z.rest:
                start = z.full * T * H
                if z.pair:
                    value = raw_ref[pl.ds(start + t * (H // 2) + h % (H // 2), D, stride=z.c2)]
                    if h >= H // 2:
                        value = pltpu.roll(value, 64, 1)
                else:
                    value = raw_ref[pl.ds(start + t * H + h, D, stride=z.c2)]
                keyed_ref[span, z.full * 128 :] = value
        scale = bound2[h : h + 1, 0:1]
        for a in range(z.NP // 128):
            for b in range(z.NP // 128):
                tile = keyed_ref[a * 128 : (a + 1) * 128, b * 128 : (b + 1) * 128].T
                plane_ref[h, b * 128 : (b + 1) * 128, a * 128 : (a + 1) * 128] = jnp.where(seen(a * 128), tile * scale, masked_score)

    if z.NP > N:
        k_ref[N:] = jnp.zeros((z.NP - N, C), bf16)
        v_ref[N:] = jnp.zeros((z.NP - N, C), bf16)

    @pl.loop(0, T)
    def _(c):
        for t in range(T):
            column_ref[t * D : (t + 1) * D] = raw_ref[pl.ds(z.p2 + t * T + c, D, stride=z.c2)]

        def inputs(b):
            span = at(b, z.JB)
            normed = (column_ref[span] * scale_n).astype(bf16)
            q_ref[span], k_ref[span], v_ref[span], g_ref[span] = project(normed, w_ref[...])

        each(N // z.JB, inputs)

        def block(b):
            span = at(b, z.JB)
            mixed = attended(z, q_ref[span], k_ref[...], v_ref[...], [plane_ref[h, span] for h in range(H)])
            gated = (g_ref[span] * mixed).astype(bf16)
            column_ref[span] = jnp.dot(gated, out_w_ref[...], preferred_element_type=f32)

        each(N // z.JB, block)
        for t in range(T):
            pay_ref[pl.ds(t * T + c, D, stride=z.c3)] = column_ref[t * D : (t + 1) * D]

    @pl.loop(0, D // 2)
    def _(device):
        send_ref[at(device, 2 * z.c3)] = pay_ref[at(device, 2 * z.c3)].astype(bf16)


def last_kernel(z, recv_ref, middle_ref, out_ref, raw_ref, row_ref):
    T, D = z.T, z.D

    @pl.loop(0, D // 2)
    def _(device):
        raw_ref[at(device, 2 * z.c3)] = recv_ref[at(device, 2 * z.c3)].astype(f32)

    @pl.loop(0, T)
    def _(t):
        for c in range(T):
            row_ref[pl.ds(c, D, stride=T)] = raw_ref[pl.ds(t * T + c, D, stride=z.c3)]
        out_ref[t] = (middle_ref[t].astype(f32) + row_ref[...]).astype(bf16)


def call(kernel, z, shapes, scratch, scalars, operands, flops, name):
    specs = [pl.BlockSpec(memory_space=pltpu.SMEM)] * scalars + [pl.BlockSpec(memory_space=pltpu.VMEM)] * (len(operands) - scalars)
    outs = [jax.ShapeDtypeStruct(shape, kind) for shape, kind in shapes]
    moved = sum(math.prod(a.shape) * a.dtype.itemsize for a in list(operands) + outs)
    return pl.pallas_call(
        functools.partial(kernel, z),
        out_shape=outs,
        in_specs=specs,
        out_specs=[pl.BlockSpec(memory_space=pltpu.VMEM)] * len(outs),
        scratch_shapes=[pltpu.VMEM(shape, kind) for shape, kind in scratch],
        cost_estimate=pl.CostEstimate(flops=flops, bytes_accessed=moved, transcendentals=0),
        compiler_params=pltpu.CompilerParams(vmem_limit_bytes=58 * 1024 * 1024),
        name=name,
    )(*operands)


def exchange(values, z, rows):
    C = values.shape[-1]
    moved = lax.all_to_all(values.reshape(z.D, rows, C), both, split_axis=0, concat_axis=0, tiled=True)
    return moved.reshape(z.D * rows, C)


def shards(
    pair_tensor,
    lengths,
    starting_gain,
    starting_weights,
    starting_bias,
    starting_output,
    ending_gain,
    ending_weights,
    ending_bias,
    ending_output,
):
    H, R = lax.axis_size("heads"), lax.axis_size("rows")
    N, C = pair_tensor.shape[1:]
    z = Sizes(N, C, R, H)
    T, D, NP, W = z.T, z.D, z.NP, z.W
    i16 = jnp.int16
    gain1, gain2 = starting_gain.reshape(1, C), ending_gain.reshape(1, C)

    planes, packed = call(
        first_plane_kernel, z,
        [((D * z.c1, C), i16), ((2 * C + 16, C), bf16)],
        [((z.L, NP), f32), ((z.c1, 128), f32)],
        0, (pair_tensor, gain1, starting_bias, starting_weights, ending_weights, ending_bias), 4 * z.L * N * C * 8, "first_plane",
    )
    planes = exchange(planes, z, z.c1)
    gathered = lax.all_gather(packed, "heads", axis=0, tiled=False)
    bias1, bias2 = gathered[:, 2 * C], gathered[:, 2 * C + 1]

    def arranged(start):
        return gathered[:, start : start + C].reshape(H, C, 4, W).transpose(1, 2, 0, 3).reshape(C, 4 * C)

    own_pair = lax.dynamic_slice_in_dim(pair_tensor, lax.axis_index("heads") * T, T, 0)
    q, k, v, g = call(
        project_kernel, z,
        [((T, N, C), bf16), ((T, NP, C), bf16), ((T, NP, C), bf16), ((T, N, C), f32)],
        [], 0, (own_pair, gain1, arranged(0)), 2 * T * N * C * 4 * C, "first_project",
    )
    middle, sent = call(
        first_node_kernel, z,
        [((T, N, C), bf16), ((D * z.c2, C), i16)],
        [((D * z.c1, 128), f32), ((H, N, NP), f32), ((N, C), f32), ((N, C), f32), ((D * z.c2, C), f32), ((up(z.p2, 8), 128), f32)],
        1, (lengths, planes, q, k, v, g, own_pair, gain1, bias1, starting_output, gain2, bias2), 4 * T * N * N * C * 2, "first_node",
    )
    received = exchange(sent, z, z.c2)
    (sent,) = call(
        second_node_kernel, z,
        [((D * z.c3, C), bf16)],
        [((D * z.c2, C), f32), ((N, C), f32), ((NP, C), bf16), ((NP, C), bf16), ((N, C), bf16), ((N, C), f32), ((NP, NP), f32), ((H, NP, NP), f32), ((D * z.c3, C), f32)],
        1, (lengths, received, arranged(C), gain2, bias2, ending_output), 4 * T * N * N * C * 2, "second_node",
    )
    received = exchange(sent, z, z.c3)
    (refined,) = call(
        last_kernel, z,
        [((T, N, C), bf16)],
        [((D * z.c3, C), f32), ((N, C), f32)],
        0, (received, middle), T * N * C, "last",
    )
    return refined


def solution(mesh):
    placed = (
        P("rows", None, None),
        P(),
        P(),
        P(None, "heads"),
        P("heads", None),
        P(),
        P(),
        P(None, "heads"),
        P("heads", None),
        P(),
    )
    return jax.shard_map(
        shards,
        mesh=mesh,
        in_specs=placed,
        out_specs=P(both, None, None),
        check_vma=False,
    )
```

```python
import functools
import math

import jax
import jax.numpy as jnp
from jax import lax
from jax.experimental import pallas as pl
from jax.experimental.pallas import tpu as pltpu
from jax.sharding import PartitionSpec as P

epsilon = 1e-05
masked_score = -1e30
log2e = math.log2(math.e)
steps = 32767.0
fine = 262143.0
f32 = jnp.float32
bf16 = jnp.bfloat16
both = ("rows", "heads")


def up(value, multiple):
    return -(-value // multiple) * multiple


class Sizes:
    def __init__(self, tokens, channels, row_devices, heads):
        self.N, self.C, self.R, self.H = tokens, channels, row_devices, heads
        self.D = row_devices * heads
        self.L = tokens // row_devices
        self.T = tokens // self.D
        self.NP = up(tokens, 128)
        self.W = channels // heads
        self.full = tokens // 128
        self.rest = tokens % 128
        self.pair = self.rest == 64
        self.p1, self.c1 = self.planes(self.L)
        self.c1 = up(self.c1 + up(self.p1, 8), 16)
        self.p2, self.c2 = self.planes(self.T * heads)
        self.low2 = up(self.p2 + self.T * self.T, 8)
        self.c2 = up(self.low2 + self.c2, 8)
        self.c3 = up(self.T * self.T, 8)
        self.small = tokens <= 256
        self.JB = tokens if self.small else 192

    def planes(self, rows):
        groups = rows // 8
        count = rows * self.full
        if self.pair:
            count += 8 * (groups // 2) + 4 * (groups % 2)
        elif self.rest:
            count += rows
        return count, 8 * (-(-(-(-count // 8)) // 5))


def each(count, body, unrolled=False):
    if count == 1 or unrolled:
        for index in range(count):
            body(index)
    else:

        @pl.loop(0, count)
        def _(index):
            body(index)


def at(index, size):
    if isinstance(index, int):
        return pl.ds(index * size, size)
    return pl.ds(pl.multiple_of(index * size, 8), size)


def nt(left, right):
    return lax.dot_general(left, right, (((1,), (1,)), ((), ())), preferred_element_type=f32)


def normalise(widened, gain):
    centre = jnp.mean(widened, axis=-1, keepdims=True)
    shifted = widened - centre
    spread = jnp.mean(shifted * shifted, axis=-1, keepdims=True)
    return (shifted * lax.rsqrt(spread + epsilon) * gain).astype(bf16)


def plane_bound(gain, bias, channels):
    product = gain * bias
    norm = jnp.sqrt(jnp.sum(product * product, axis=-1, keepdims=True))
    return jnp.maximum(norm * (1.01 * math.sqrt(channels)), 1e-20)


def normed_bound(gain, channels):
    return jnp.max(jnp.abs(gain), axis=-1, keepdims=True) * (1.01 * math.sqrt(channels))


def lanes(rows=8):
    return lax.broadcasted_iota(jnp.int32, (rows, 128), 1)


def sublanes():
    return lax.broadcasted_iota(jnp.int32, (8, 128), 0)


def plane_blocks(z, values):
    groups = values.shape[0] // 8
    blocks = [values[g * 8 : g * 8 + 8, n * 128 : n * 128 + 128] for n in range(z.full) for g in range(groups)]
    if z.rest:
        last = [values[g * 8 : g * 8 + 8, z.full * 128 :] for g in range(groups)]
        if z.pair:
            for g in range(0, groups - 1, 2):
                blocks.append(jnp.where(lanes() < 64, last[g], pltpu.roll(last[g + 1], 64, 1)))
            if groups % 2:
                blocks.append(jnp.where(lanes() < 64, last[-1], pltpu.roll(pltpu.roll(last[-1], 64, 1), 4, 0)))
        else:
            blocks += last
    high, low = [], []
    for n, block in enumerate(blocks):
        whole = jnp.round(block).astype(jnp.int32)
        upper = (whole + 4) >> 3
        digit = (whole - upper * 8 + 4) << (3 * (n % 5))
        high.append(upper.astype(f32))
        low = low + [digit] if n % 5 == 0 else low[:-1] + [low[-1] + digit]
    return high, [block.astype(f32) for block in low]


def whole_value(high, low, number):
    return (high * 8 + ((low >> (3 * (number % 5))) & 7) - 4).astype(f32)


def first_plane_kernel(
    z, head_ref, pair_ref, gain_ref, bias_ref, w1_ref, w2_ref, b2_ref, out_ref, weights_ref, own_ref, normed_ref, wide_ref, plane_ref
):
    N, C, L, T = z.N, z.C, z.L, z.T
    gain = gain_ref[...]
    bias = bias_ref[...].astype(f32)
    weights_ref[0:C] = w1_ref[...]
    weights_ref[C : 2 * C] = w2_ref[...]
    row = lax.broadcasted_iota(jnp.int32, (16, C), 0)
    weights_ref[2 * C : 2 * C + 16] = jnp.where(row == 0, bias, b2_ref[...].astype(f32)).astype(bf16)

    @pl.loop(0, L // 8)
    def _(group):
        for j in range(8):
            normed = normalise(pair_ref[group * 8 + j].astype(f32), gain)
            wide_ref[:, pl.ds(pl.multiple_of((group * 8 + j) * C, 128), C)] = normed

    row = lax.broadcasted_iota(jnp.int32, (L, C), 0)
    left = jnp.concatenate([jnp.where(row == j, bias, 0.0).astype(bf16) for j in range(L)], axis=1)
    plane_ref[:, 0:N] = nt(left, wide_ref[...]) * (fine / plane_bound(gain, bias, C))
    high, low = plane_blocks(z, plane_ref[...])
    spare = [jnp.zeros((8, 128), f32)] * (z.c1 // 8 - len(high) - len(low))
    chunk = jnp.concatenate(high + low + spare, axis=0).astype(jnp.int32).astype(jnp.int16)

    @pl.loop(0, z.D)
    def _(device):
        out_ref[pl.ds(pl.multiple_of(device * z.c1, 16), z.c1)] = chunk

    first = head_ref[0] * T
    for t in range(T):
        own_ref[t] = pair_ref[first + t]
        normed_ref[t] = wide_ref[:, pl.ds(pl.multiple_of((first + t) * C, 128), C)]


def arranged(z, gathered_ref, start):
    C, W = z.C, z.W
    lane = lax.broadcasted_iota(jnp.int32, (C, C), 1)
    own = [gathered_ref[h, start : start + C].astype(f32) for h in range(z.H)]
    kinds = []
    for kind in range(4):
        value = own[0] if kind == 0 else pltpu.roll(own[0], (C - kind * W) % C, 1)
        for h in range(1, z.H):
            moved = own[h] if h == kind else pltpu.roll(own[h], ((h - kind) * W) % C, 1)
            value = jnp.where(lane < h * W, value, moved)
        kinds.append(value.astype(bf16))
    return jnp.concatenate(kinds, axis=1)


def project(normed, weights):
    C = normed.shape[1]
    projected = jnp.dot(normed, weights, preferred_element_type=f32)
    queries, keys, values = (projected[:, n * C : (n + 1) * C].astype(bf16) for n in range(3))
    gates = 1.0 / (1.0 + jnp.exp(-projected[:, 3 * C :]))
    return queries, keys, values, gates


def project_kernel(z, normed_ref, gathered_ref, q_ref, k_ref, v_ref, g_ref, bias_ref):
    C = z.C
    weights = arranged(z, gathered_ref, 0)
    rows = [gathered_ref[h, 2 * C : 2 * C + 16].astype(f32) for h in range(z.H)]
    bias_ref[...] = jnp.zeros_like(bias_ref)
    for h in range(z.H):
        bias_ref[h : h + 1] = rows[h][0:1]
        bias_ref[z.H + h : z.H + h + 1] = rows[h][1:2]

    def row(t):
        def block(b):
            span = at(b, z.JB)
            q_ref[t, span], k_ref[t, span], v_ref[t, span], g_ref[t, span] = project(normed_ref[t, span], weights)

        each(z.N // z.JB, block)
        if z.NP > z.N:
            k_ref[t, z.N :] = jnp.zeros((z.NP - z.N, C), bf16)
            v_ref[t, z.N :] = jnp.zeros((z.NP - z.N, C), bf16)

    each(z.T, row, z.small)


def arrange_kernel(z, gathered_ref, out_ref):
    out_ref[...] = arranged(z, gathered_ref, z.C)


def head_masks(z):
    lane = lax.broadcasted_iota(jnp.int32, (1, z.C), 1)
    return [jnp.where((lane >= h * z.W) & (lane < (h + 1) * z.W), 1.0, 0.0).astype(bf16) for h in range(z.H)]


def attended(z, queries, keys, values, planes):
    masks = head_masks(z)
    rows = queries.shape[0]
    stacked = jnp.concatenate([queries * mask for mask in masks], axis=0)
    scores = nt(stacked, keys) * (log2e / math.sqrt(z.W))
    parts = []
    for h in range(z.H):
        score = scores[h * rows : (h + 1) * rows] + planes[h]
        raised = jnp.exp2(score - jnp.max(score, axis=-1, keepdims=True))
        parts.append((raised * (1.0 / jnp.sum(raised, axis=-1, keepdims=True))).astype(bf16))
    return jnp.dot(
        jnp.concatenate(parts, axis=1),
        jnp.concatenate([values * mask for mask in masks], axis=0),
        preferred_element_type=f32,
    )


def first_node_kernel(
    z, lengths_ref, recv_ref, q_ref, k_ref, v_ref, g_ref, pair_ref, bias_ref, gain1_ref, out_w_ref, gain2_ref,
    middle_ref, send_ref, plane_ref, row_ref, wide_ref, own_ref, pay_ref,
):
    N, T, H, D, L, C = z.N, z.T, z.H, z.D, z.L, z.C
    length = lengths_ref[0]
    bound1 = plane_bound(gain1_ref[...], bias_ref[0:H], C) * (log2e / fine)
    gain2 = gain2_ref[...]
    factor_n = steps / normed_bound(gain2, C)
    blocks = up(z.p1, 8) // 8
    groups = L // 8
    seen = [lanes() + n * 128 < length for n in range(z.full)]
    seen_rest = (lanes() + z.full * 128 < length) & (lanes() < z.rest)

    @pl.loop(0, z.R)
    def _(r):
        for h in range(H):
            scale = bound1[h : h + 1, 0:1]
            chunk = recv_ref[pl.ds(pl.multiple_of((r * H + h) * z.c1, 16), z.c1)].astype(jnp.int32)
            low = [chunk[(blocks + n) * 8 : (blocks + n) * 8 + 8] for n in range(-(-blocks // 5))]
            value = [whole_value(chunk[n * 8 : n * 8 + 8], low[n // 5], n) * scale for n in range(blocks)]
            for g in range(groups):
                target = pl.ds(pl.multiple_of(r * L + g * 8, 8), 8)
                for n in range(z.full):
                    plane_ref[h, target, n * 128 : n * 128 + 128] = jnp.where(seen[n], value[n * groups + g], masked_score)
                if z.rest:
                    base = z.full * groups
                    if not z.pair:
                        last = value[base + g]
                    elif g == groups - 1 and g % 2 == 0:
                        last = value[base + g // 2]
                        last = jnp.where(sublanes() < 4, last, pltpu.roll(pltpu.roll(last, 64, 1), 4, 0))
                    else:
                        last = value[base + g // 2]
                        last = pltpu.roll(last, 64, 1) if g % 2 else last
                    plane_ref[h, target, z.full * 128 :] = jnp.where(seen_rest, last, masked_score)

    def row(t):
        def block(b):
            span = at(b, z.JB)
            mixed = attended(z, q_ref[t, span], k_ref[t], v_ref[t], [plane_ref[h, span] for h in range(H)])
            gated = (g_ref[t, span] * mixed).astype(bf16)
            update = jnp.dot(gated, out_w_ref[...], preferred_element_type=f32)
            middle = (pair_ref[t, span].astype(f32) + update).astype(bf16)
            middle_ref[t, span] = middle
            row_ref[t, span] = normalise(middle.astype(f32), gain2).astype(f32)

        each(N // z.JB, block)
        for c in range(T):
            piece = row_ref[t, pl.ds(c, D, stride=T)]
            lane = t * C if isinstance(t, int) else pl.multiple_of(t * C, 128)
            wide_ref[c * D : (c + 1) * D, pl.ds(lane, C)] = piece.astype(bf16)
            pay_ref[pl.ds(z.p2 + t * T + c, D, stride=z.c2)] = jnp.round(piece * factor_n)

    each(T, row, z.small)
    bias2 = bias_ref[H : 2 * H]
    repeated = jnp.concatenate([bias2] * T, axis=0)
    line = lax.broadcasted_iota(jnp.int32, (T * H, C), 0)
    left = jnp.concatenate([jnp.where((line >= t * H) & (line < (t + 1) * H), repeated, 0.0).astype(bf16) for t in range(T)], axis=1)
    own_ref[:, 0:N] = nt(left, wide_ref[...]) * (fine / plane_bound(gain2, repeated, C))
    high, low = plane_blocks(z, own_ref[...])
    high = jnp.concatenate(high, axis=0)[0 : z.p2]
    low = jnp.concatenate(low, axis=0)

    @pl.loop(0, D)
    def _(device):
        pay_ref[pl.ds(pl.multiple_of(device * z.c2, 8), z.p2)] = high
        pay_ref[pl.ds(pl.multiple_of(device * z.c2 + z.low2, 8), low.shape[0])] = low

    @pl.loop(0, D // 2)
    def _(device):
        send_ref[at(device, 2 * z.c2)] = pay_ref[at(device, 2 * z.c2)].astype(jnp.int32).astype(jnp.int16)


def second_node_kernel(
    z, lengths_ref, recv_ref, w_ref, bias_ref, gain2_ref, out_w_ref,
    send_ref, raw_ref, column_ref, q_ref, k_ref, v_ref, g_ref, keyed_ref, plane_ref, pay_ref,
):
    N, T, H, D, C = z.N, z.T, z.H, z.D, z.C
    length = lengths_ref[0]
    gain2 = gain2_ref[...]
    bound2 = plane_bound(gain2, bias_ref[H : 2 * H], C) * (log2e / fine)
    scale_n = normed_bound(gain2, C) * (1.0 / steps)
    blocks = up(z.p2, 8) // 8

    @pl.loop(0, D // 2)
    def _(pair):
        both_chunks = recv_ref[at(pair, 2 * z.c2)].astype(jnp.int32)
        for half in range(2):
            chunk = both_chunks[half * z.c2 : (half + 1) * z.c2]
            start = pl.multiple_of(pair * (2 * z.c2) + half * z.c2, 8)
            for n in range(blocks):
                high = chunk[n * 8 : n * 8 + 8]
                value = whole_value(high, chunk[z.low2 + n // 5 * 8 : z.low2 + n // 5 * 8 + 8], n)
                if (n + 1) * 8 > z.p2:
                    value = jnp.where(sublanes() < z.p2 - n * 8, value, high.astype(f32))
                raw_ref[pl.ds(start + n * 8, 8)] = value
            raw_ref[pl.ds(start + blocks * 8, z.low2 - blocks * 8)] = chunk[blocks * 8 : z.low2].astype(f32)

    def normed_rows(c):
        for t in range(T):
            piece = raw_ref[pl.ds(z.p2 + t * T + c, D, stride=z.c2)]
            column_ref[c, t * D : (t + 1) * D] = (piece * scale_n).astype(bf16)

        def inputs(b):
            span = at(b, z.JB)
            q_ref[c, span], k_ref[c, span], v_ref[c, span], g_ref[c, span] = project(column_ref[c, span], w_ref[...])

        each(N // z.JB, inputs)
        if z.NP > N:
            k_ref[c, N:] = jnp.zeros((z.NP - N, C), bf16)
            v_ref[c, N:] = jnp.zeros((z.NP - N, C), bf16)

    each(T, normed_rows, z.small)

    def seen(base):
        slot = lax.broadcasted_iota(jnp.int32, (1, 128), 1) + base
        return ((slot % D) * T + slot // D < length) & (slot < N)

    for h in range(H):
        for t in range(T):
            span = pl.ds(t * D, D)
            line = t * H + h
            for n in range(z.full):
                keyed_ref[h, span, n * 128 : (n + 1) * 128] = raw_ref[pl.ds(n * T * H + line, D, stride=z.c2)]
            if z.rest:
                place, turned = line, False
                if z.pair:
                    group, groups = line // 8, T * H // 8
                    if group == groups - 1 and groups % 2:
                        place, turned = group // 2 * 8 + line % 4, line % 8 >= 4
                    else:
                        place, turned = group // 2 * 8 + line % 8, group % 2 == 1
                value = raw_ref[pl.ds(z.full * T * H + place, D, stride=z.c2)]
                keyed_ref[h, span, z.full * 128 :] = pltpu.roll(value, 64, 1) if turned else value
        scale = bound2[h : h + 1, 0:1]
        for a in range(z.NP // 128):
            for b in range(z.NP // 128):
                tile = keyed_ref[h, a * 128 : (a + 1) * 128, b * 128 : (b + 1) * 128].T
                plane_ref[h, b * 128 : (b + 1) * 128, a * 128 : (a + 1) * 128] = jnp.where(seen(a * 128), tile * scale, masked_score)

    def column(c):
        def block(b):
            span = at(b, z.JB)
            mixed = attended(z, q_ref[c, span], k_ref[c], v_ref[c], [plane_ref[h, span] for h in range(H)])
            gated = (g_ref[c, span] * mixed).astype(bf16)
            g_ref[c, span] = jnp.dot(gated, out_w_ref[...], preferred_element_type=f32)

        each(N // z.JB, block)
        for t in range(T):
            pay_ref[pl.ds(t * T + c, D, stride=z.c3)] = g_ref[c, t * D : (t + 1) * D]

    each(T, column, z.small)

    @pl.loop(0, D // 2)
    def _(device):
        send_ref[at(device, 2 * z.c3)] = pay_ref[at(device, 2 * z.c3)].astype(bf16)


def last_kernel(z, recv_ref, middle_ref, out_ref, raw_ref, row_ref):
    T, D = z.T, z.D

    @pl.loop(0, D // 2)
    def _(device):
        raw_ref[at(device, 2 * z.c3)] = recv_ref[at(device, 2 * z.c3)].astype(f32)

    for t in range(T):
        for c in range(T):
            row_ref[t, pl.ds(c, D, stride=T)] = raw_ref[pl.ds(t * T + c, D, stride=z.c3)]
        out_ref[t] = (middle_ref[t].astype(f32) + row_ref[t]).astype(bf16)


def call(kernel, z, shapes, scratch, scalars, operands, flops, room=16 * 2**20):
    name = kernel.__name__
    specs = [pl.BlockSpec(memory_space=pltpu.SMEM)] * scalars + [pl.BlockSpec(memory_space=pltpu.VMEM)] * (len(operands) - scalars)
    outs = [jax.ShapeDtypeStruct(shape, kind) for shape, kind in shapes]
    size = lambda shape, kind: math.prod(shape) * jnp.dtype(kind).itemsize
    moved = sum(size(a.shape, a.dtype) for a in list(operands) + outs)
    held = moved + sum(size(shape, kind) for shape, kind in scratch)
    return pl.pallas_call(
        functools.partial(kernel, z),
        out_shape=outs,
        in_specs=specs,
        out_specs=[pl.BlockSpec(memory_space=pltpu.VMEM)] * len(outs),
        scratch_shapes=[pltpu.VMEM(shape, kind) for shape, kind in scratch],
        cost_estimate=pl.CostEstimate(flops=flops, bytes_accessed=moved, transcendentals=0),
        compiler_params=pltpu.CompilerParams(vmem_limit_bytes=min(58 * 2**20, 2 * held + room)),
        name=name,
    )(*operands)


def exchange(values, z, rows):
    C = values.shape[-1]
    moved = lax.all_to_all(values.reshape(z.D, rows, C), both, split_axis=0, concat_axis=0, tiled=True)
    return moved.reshape(z.D * rows, C)


def shards(
    pair_tensor,
    lengths,
    starting_gain,
    starting_weights,
    starting_bias,
    starting_output,
    ending_gain,
    ending_weights,
    ending_bias,
    ending_output,
):
    H, R = lax.axis_size("heads"), lax.axis_size("rows")
    N, C = pair_tensor.shape[1:]
    z = Sizes(N, C, R, H)
    T, D, NP = z.T, z.D, z.NP
    i16 = jnp.int16
    gain1, gain2 = starting_gain.reshape(1, C), ending_gain.reshape(1, C)
    head = lax.axis_index("heads").astype(jnp.int32).reshape(1)

    planes, packed, own_pair, normed = call(
        first_plane_kernel, z,
        [((D * z.c1, C), i16), ((2 * C + 16, C), bf16), ((T, N, C), bf16), ((T, N, C), bf16)],
        [((N, z.L * C), bf16), ((z.L, NP), f32)],
        1, (head, pair_tensor, gain1, starting_bias, starting_weights, ending_weights, ending_bias), 2 * z.L * N * C * 8, 58 * 2**20,
    )
    planes = exchange(planes, z, z.c1)
    gathered = lax.all_gather(packed, "heads", axis=0, tiled=False)
    q, k, v, g, biases = call(
        project_kernel, z,
        [((T, N, C), bf16), ((T, NP, C), bf16), ((T, NP, C), bf16), ((T, N, C), f32), ((up(2 * H, 8), C), f32)],
        [], 0, (normed, gathered), 2 * T * N * C * 4 * C,
    )
    middle, sent = call(
        first_node_kernel, z,
        [((T, N, C), bf16), ((D * z.c2, C), i16)],
        [((H, N, NP), f32), ((T, N, C), f32), ((N, T * C), bf16), ((T * H, NP), f32), ((D * z.c2, C), f32)],
        1, (lengths, planes, q, k, v, g, own_pair, biases, gain1, starting_output, gain2), 4 * T * N * N * C * 2,
    )
    received = exchange(sent, z, z.c2)
    (weights2,) = call(arrange_kernel, z, [((C, 4 * C), bf16)], [], 0, (gathered,), 4 * C * C)
    (sent,) = call(
        second_node_kernel, z,
        [((D * z.c3, C), bf16)],
        [
            ((D * z.c2, C), f32), ((T, N, C), bf16), ((T, N, C), bf16), ((T, NP, C), bf16), ((T, NP, C), bf16), ((T, N, C), f32),
            ((H, NP, NP), f32), ((H, NP, NP), f32), ((D * z.c3, C), f32),
        ],
        1, (lengths, received, weights2, biases, gain2, ending_output), 4 * T * N * N * C * 2,
    )
    received = exchange(sent, z, z.c3)
    (refined,) = call(
        last_kernel, z, [((T, N, C), bf16)], [((D * z.c3, C), f32), ((T, N, C), f32)], 0, (received, middle), T * N * C
    )
    return refined


def solution(mesh):
    placed = (
        P("rows", None, None),
        P(),
        P(),
        P(None, "heads"),
        P("heads", None),
        P(),
        P(),
        P(None, "heads"),
        P("heads", None),
        P(),
    )
    return jax.shard_map(
        shards,
        mesh=mesh,
        in_specs=placed,
        out_specs=P(both, None, None),
        check_vma=False,
    )
```

```python
import functools
import math

import jax
import jax.numpy as jnp
from jax import lax
from jax.experimental import pallas as pl
from jax.experimental.pallas import tpu as pltpu
from jax.sharding import PartitionSpec as P

epsilon = 1e-05
masked_score = -1e30
log2e = math.log2(math.e)
steps = 32767.0
fine = 262143.0
f32 = jnp.float32
bf16 = jnp.bfloat16
both = ("rows", "heads")


def up(value, multiple):
    return -(-value // multiple) * multiple


class Sizes:
    def __init__(self, tokens, channels, row_devices, heads):
        self.N, self.C, self.R, self.H = tokens, channels, row_devices, heads
        self.D = row_devices * heads
        self.L = tokens // row_devices
        self.T = tokens // self.D
        self.NP = up(tokens, 128)
        self.W = channels // heads
        self.full = tokens // 128
        self.rest = tokens % 128
        self.pair = self.rest == 64
        self.p1, self.c1 = self.planes(self.L)
        self.c1 = up(self.p1, 8)
        self.p2, self.c2 = self.planes(self.T * heads)
        self.low2 = up(self.p2 + self.T * self.T, 8)
        self.c2 = up(self.low2 + self.c2, 8)
        self.c3 = up(self.T * self.T, 8)
        self.small = tokens <= 256
        self.JB = tokens if self.small else 192

    def planes(self, rows):
        groups = rows // 8
        count = rows * self.full
        if self.pair:
            count += 8 * (groups // 2) + 4 * (groups % 2)
        elif self.rest:
            count += rows
        return count, 8 * (-(-(-(-count // 8)) // 5))


def each(count, body, unrolled=False):
    if count == 1 or unrolled:
        for index in range(count):
            body(index)
    else:

        @pl.loop(0, count)
        def _(index):
            body(index)


def at(index, size):
    if isinstance(index, int):
        return pl.ds(index * size, size)
    return pl.ds(pl.multiple_of(index * size, 8), size)


def nt(left, right):
    return lax.dot_general(left, right, (((1,), (1,)), ((), ())), preferred_element_type=f32)


def normalise(widened, gain):
    centre = jnp.mean(widened, axis=-1, keepdims=True)
    shifted = widened - centre
    spread = jnp.mean(shifted * shifted, axis=-1, keepdims=True)
    return (shifted * lax.rsqrt(spread + epsilon) * gain).astype(bf16)


def plane_bound(gain, bias, channels):
    product = gain * bias
    norm = jnp.sqrt(jnp.sum(product * product, axis=-1, keepdims=True))
    return jnp.maximum(norm * (1.01 * math.sqrt(channels)), 1e-20)


def normed_bound(gain, channels):
    return jnp.max(jnp.abs(gain), axis=-1, keepdims=True) * (1.01 * math.sqrt(channels))


def lanes(rows=8):
    return lax.broadcasted_iota(jnp.int32, (rows, 128), 1)


def sublanes():
    return lax.broadcasted_iota(jnp.int32, (8, 128), 0)


def plane_blocks(z, values):
    groups = values.shape[0] // 8
    blocks = [values[g * 8 : g * 8 + 8, n * 128 : n * 128 + 128] for n in range(z.full) for g in range(groups)]
    if z.rest:
        last = [values[g * 8 : g * 8 + 8, z.full * 128 :] for g in range(groups)]
        if z.pair:
            for g in range(0, groups - 1, 2):
                blocks.append(jnp.where(lanes() < 64, last[g], pltpu.roll(last[g + 1], 64, 1)))
            if groups % 2:
                blocks.append(jnp.where(lanes() < 64, last[-1], pltpu.roll(pltpu.roll(last[-1], 64, 1), 4, 0)))
        else:
            blocks += last
    return blocks


def digits(blocks):
    high, low = [], []
    for n, block in enumerate(blocks):
        whole = jnp.round(block).astype(jnp.int32)
        upper = (whole + 4) >> 3
        digit = (whole - upper * 8 + 4) << (3 * (n % 5))
        high.append(upper.astype(f32))
        low = low + [digit] if n % 5 == 0 else low[:-1] + [low[-1] + digit]
    return high, [block.astype(f32) for block in low]


def whole_value(high, low, number):
    return (high * 8 + ((low >> (3 * (number % 5))) & 7) - 4).astype(f32)


def log_scale(gain, bias, channels):
    return 65535.0 / jnp.log(1.0 + 2.0 * jnp.maximum(plane_bound(gain, bias, channels), 1e-3))


def first_plane_kernel(
    z, head_ref, lengths_ref, gain_far, bias_far, b2_far, w1_ref, pair_ref,
    out_ref, weights_ref, normed_ref, held_ref, wide_ref, plane_ref, twice_ref, pack_ref, gain_ref, bias_ref, b2_ref,
    arrived, left_sem, sent_sem, w_sem,
):
    N, C, L, T = z.N, z.C, z.L, z.T
    copies = [pltpu.make_async_copy(pair_ref.at[at(g, 8)], held_ref.at[at(g, 8)], arrived.at[g]) for g in range(L // 8)]
    small = ((gain_far, gain_ref), (bias_far, bias_ref), (b2_far, b2_ref), (w1_ref, pack_ref.at[pl.ds(0, C)]))
    small = [pltpu.make_async_copy(there, here, w_sem.at[n]) for n, (there, here) in enumerate(small)]
    for copy in small[:1] + copies + small[1:]:
        copy.start()
    small[0].wait()
    gain = gain_ref[...]
    for group in range(L // 8):
        copies[group].wait()
        for j in range(group * 8, group * 8 + 8):
            wide_ref[:, j * C : (j + 1) * C] = normalise(held_ref[j].astype(f32), gain)
    for copy in small[1:]:
        copy.wait()
    bias = bias_ref[...].astype(f32)
    row = lax.broadcasted_iota(jnp.int32, (16, C), 0)
    pack_ref[C : C + 16] = jnp.where(row == 0, bias, b2_ref[...].astype(f32)).astype(bf16)
    first = head_ref[0] * T
    sends = [pltpu.make_async_copy(pack_ref, weights_ref, w_sem.at[4])]
    for t in range(T):
        own = wide_ref.at[:, pl.ds(pl.multiple_of((first + t) * C, 128), C)]
        sends.append(pltpu.make_async_copy(own, normed_ref.at[t], left_sem.at[t]))
    for send in sends:
        send.start()

    row = lax.broadcasted_iota(jnp.int32, (L, C), 0)
    left = jnp.concatenate([jnp.where(row == j, bias, 0.0).astype(bf16) for j in range(L)], axis=1)
    plane_ref[:, 0:N] = nt(left, wide_ref[...])
    slot = lax.broadcasted_iota(jnp.int32, (L, z.NP), 1)
    plane = jnp.where((slot < lengths_ref[0]) & (slot < N), plane_ref[...], masked_score)
    below = jnp.max(plane, axis=-1, keepdims=True) - plane
    below = jnp.where(below < 1e20, below, 0.0)
    code = jnp.round(jnp.log(1.0 + below) * log_scale(gain, bias, C)) - 32768.0
    blocks = jnp.concatenate(plane_blocks(z, code), axis=0).astype(jnp.int32)
    twice_ref[...] = jnp.concatenate([blocks, blocks], axis=0).astype(jnp.int16)
    for n in range(z.D // 2):
        sends.append(pltpu.make_async_copy(twice_ref, out_ref.at[at(n, 2 * z.c1)], sent_sem.at[n]))
        sends[-1].start()
    for send in sends:
        send.wait()


def arranged(z, columns):
    C, W, H = z.C, z.W, z.H
    lane = lax.broadcasted_iota(jnp.int32, (C, C), 1)
    own = [column.astype(f32) for column in columns]
    parts = []
    for kind in range(4):
        moved = [own[h] if h == kind else pltpu.roll(own[h], ((h - kind) * W) % C, 1) for h in range(H)]
        alone = [jnp.where((lane >= h * W) & (lane < (h + 1) * W), moved[h], 0.0) for h in range(H)]
        parts += [sum(alone[1:], alone[0])] if kind else alone
    return jnp.concatenate([part.astype(bf16) for part in parts], axis=1)


def project(z, normed, weights, t, span, q_ref, k_ref, v_ref, g_ref):
    C, H = z.C, z.H
    projected = jnp.dot(normed, weights, preferred_element_type=f32)
    part = lambda n: projected[:, n * C : (n + 1) * C]
    for h in range(H):
        q_ref[t, h, span] = part(h).astype(bf16)
    k_ref[t, span] = part(H).astype(bf16)
    v_ref[t, span] = part(H + 1).astype(bf16)
    g_ref[t, span] = 1.0 / (1.0 + jnp.exp(-part(H + 2)))


def padding(z, t, k_ref, v_ref):
    if z.NP > z.N:
        k_ref[t, z.N :] = jnp.zeros((z.NP - z.N, z.C), bf16)
        v_ref[t, z.N :] = jnp.zeros((z.NP - z.N, z.C), bf16)


def project_kernel(z, gathered_ref, normed_ref, q_ref, k_ref, v_ref, g_ref, bias_ref, held_ref, arrived):
    C = z.C
    copy = pltpu.make_async_copy(normed_ref, held_ref, arrived.at[0])
    copy.start()
    weights = arranged(z, [gathered_ref[h, 0:C] for h in range(z.H)])
    rows = [gathered_ref[h, C : C + 16].astype(f32) for h in range(z.H)]
    bias_ref[...] = jnp.zeros_like(bias_ref)
    for h in range(z.H):
        bias_ref[h : h + 1] = rows[h][0:1]
        bias_ref[z.H + h : z.H + h + 1] = rows[h][1:2]
    copy.wait()

    def row(t):
        def block(b):
            span = at(b, z.JB)
            project(z, held_ref[t, span], weights, t, span, q_ref, k_ref, v_ref, g_ref)

        each(z.N // z.JB, block, z.small)
        padding(z, t, k_ref, v_ref)

    each(z.T, row, z.small)


def arrange_kernel(z, gathered_ref, out_ref):
    out_ref[...] = arranged(z, [gathered_ref[h] for h in range(z.H)])


def attended(z, queries, keys, values, planes):
    rows = planes[0].shape[0]
    scores = nt(queries, keys) * (log2e / math.sqrt(z.W))
    parts = []
    for h in range(z.H):
        score = scores[h * rows : (h + 1) * rows] + planes[h]
        raised = jnp.exp2(score - jnp.max(score, axis=-1, keepdims=True))
        parts.append((raised * (1.0 / jnp.sum(raised, axis=-1, keepdims=True))).astype(bf16))
    sums = jnp.dot(jnp.concatenate(parts, axis=0), values, preferred_element_type=f32)
    lane = lax.broadcasted_iota(jnp.int32, (rows, z.C), 1)
    result = sums[(z.H - 1) * rows :]
    for h in range(z.H - 2, -1, -1):
        result = jnp.where(lane < (h + 1) * z.W, sums[h * rows : (h + 1) * rows], result)
    return result


def mixed(z, t, span, q_ref, k_ref, v_ref, plane_ref):
    queries = jnp.concatenate([q_ref[t, h, span] for h in range(z.H)], axis=0)
    return attended(z, queries, k_ref[t], v_ref[t], [plane_ref[h, span] for h in range(z.H)])


def first_node_kernel(
    z, head_ref, lengths_ref, recv_ref, q_ref, k_ref, v_ref, g_ref, bias_ref, gain1_ref, out_w_ref, gain2_ref, whole_ref,
    middle_out, send_out, plane_ref, row_ref, wide_ref, own_ref, pay_ref, pair_ref, middle_ref, send_ref, arrived, sent_sem,
):
    N, T, H, D, L, C = z.N, z.T, z.H, z.D, z.L, z.C
    length = lengths_ref[0]
    copy = pltpu.make_async_copy(whole_ref.at[pl.ds(head_ref[0] * T, T)], pair_ref, arrived.at[0])
    copy.start()
    unit = 1.0 / log_scale(gain1_ref[...], bias_ref[0:H], C)
    gain2 = gain2_ref[...]
    factor_n = steps / normed_bound(gain2, C)
    blocks = up(z.p1, 8) // 8
    groups = L // 8
    seen = [lanes() + n * 128 < length for n in range(z.full)]
    seen_rest = (lanes() + z.full * 128 < length) & (lanes() < z.rest)

    @pl.loop(0, z.R)
    def _(r):
        chunks = recv_ref[at(r, H * z.c1)].astype(jnp.int32)
        for h in range(H):
            chunk = chunks[h * z.c1 : (h + 1) * z.c1].astype(f32)
            value = (1.0 - jnp.exp((chunk + 32768.0) * unit[h : h + 1, 0:1])) * log2e
            value = [value[n * 8 : n * 8 + 8] for n in range(blocks)]
            for g in range(groups):
                target = pl.ds(pl.multiple_of(r * L + g * 8, 8), 8)
                for n in range(z.full):
                    plane_ref[h, target, n * 128 : n * 128 + 128] = jnp.where(seen[n], value[n * groups + g], masked_score)
                if z.rest:
                    base = z.full * groups
                    if not z.pair:
                        last = value[base + g]
                    elif g == groups - 1 and g % 2 == 0:
                        last = value[base + g // 2]
                        last = jnp.where(sublanes() < 4, last, pltpu.roll(pltpu.roll(last, 64, 1), 4, 0))
                    else:
                        last = value[base + g // 2]
                        last = pltpu.roll(last, 64, 1) if g % 2 else last
                    plane_ref[h, target, z.full * 128 :] = jnp.where(seen_rest, last, masked_score)

    copy.wait()

    def row(t):
        def block(b):
            span = at(b, z.JB)
            gated = (g_ref[t, span] * mixed(z, t, span, q_ref, k_ref, v_ref, plane_ref)).astype(bf16)
            update = jnp.dot(gated, out_w_ref[...], preferred_element_type=f32)
            middle = (pair_ref[t, span].astype(f32) + update).astype(bf16)
            middle_ref[t, span] = middle
            row_ref[t, span] = normalise(middle.astype(f32), gain2).astype(f32)

        each(N // z.JB, block, z.small)
        for c in range(T):
            piece = row_ref[t, pl.ds(c, D, stride=T)]
            lane = t * C if isinstance(t, int) else pl.multiple_of(t * C, 128)
            wide_ref[c * D : (c + 1) * D, pl.ds(lane, C)] = piece.astype(bf16)
            pay_ref[pl.ds(z.p2 + t * T + c, D, stride=z.c2)] = jnp.round(piece * factor_n)

    each(T, row, z.small)
    sends = [pltpu.make_async_copy(middle_ref, middle_out, sent_sem.at[0])]
    sends[0].start()
    bias2 = bias_ref[H : 2 * H]
    repeated = jnp.concatenate([bias2] * T, axis=0)
    line = lax.broadcasted_iota(jnp.int32, (T * H, C), 0)
    left = jnp.concatenate([jnp.where((line >= t * H) & (line < (t + 1) * H), repeated, 0.0).astype(bf16) for t in range(T)], axis=1)
    own_ref[:, 0:N] = nt(left, wide_ref[...]) * (fine / plane_bound(gain2, repeated, C))
    high, low = digits(plane_blocks(z, own_ref[...]))
    high = jnp.concatenate(high, axis=0)[0 : z.p2]
    low = jnp.concatenate(low, axis=0)

    share = D // 4
    for n in range(4):

        @pl.loop(n * share, (n + 1) * share)
        def _(device):
            pay_ref[pl.ds(pl.multiple_of(device * z.c2, 8), z.p2)] = high
            pay_ref[pl.ds(pl.multiple_of(device * z.c2 + z.low2, 8), low.shape[0])] = low

        @pl.loop(n * share // 2, (n + 1) * share // 2)
        def _(device):
            send_ref[at(device, 2 * z.c2)] = pay_ref[at(device, 2 * z.c2)].astype(jnp.int32).astype(jnp.int16)

        span = at(n, share * z.c2)
        sends.append(pltpu.make_async_copy(send_ref.at[span], send_out.at[span], sent_sem.at[1 + n]))
        sends[-1].start()
    for send in sends:
        send.wait()


def second_node_kernel(
    z, lengths_ref, recv_ref, w_ref, bias_ref, gain2_ref, out_w_ref,
    send_ref, raw_ref, column_ref, q_ref, k_ref, v_ref, g_ref, keyed_ref, plane_ref, pay_ref,
):
    N, T, H, D, C = z.N, z.T, z.H, z.D, z.C
    length = lengths_ref[0]
    gain2 = gain2_ref[...]
    bound2 = plane_bound(gain2, bias_ref[H : 2 * H], C) * (log2e / fine)
    scale_n = normed_bound(gain2, C) * (1.0 / steps)
    blocks = up(z.p2, 8) // 8

    @pl.loop(0, D // 2)
    def _(pair):
        both_chunks = recv_ref[at(pair, 2 * z.c2)].astype(jnp.int32)
        for half in range(2):
            chunk = both_chunks[half * z.c2 : (half + 1) * z.c2]
            start = pl.multiple_of(pair * (2 * z.c2) + half * z.c2, 8)
            for n in range(blocks):
                high = chunk[n * 8 : n * 8 + 8]
                value = whole_value(high, chunk[z.low2 + n // 5 * 8 : z.low2 + n // 5 * 8 + 8], n)
                if (n + 1) * 8 > z.p2:
                    value = jnp.where(sublanes() < z.p2 - n * 8, value, high.astype(f32))
                raw_ref[pl.ds(start + n * 8, 8)] = value
            raw_ref[pl.ds(start + blocks * 8, z.low2 - blocks * 8)] = chunk[blocks * 8 : z.low2].astype(f32)

    def normed_rows(c):
        for t in range(T):
            piece = raw_ref[pl.ds(z.p2 + t * T + c, D, stride=z.c2)]
            column_ref[c, t * D : (t + 1) * D] = (piece * scale_n).astype(bf16)

        def inputs(b):
            span = at(b, z.JB)
            project(z, column_ref[c, span], w_ref[...], c, span, q_ref, k_ref, v_ref, g_ref)

        each(N // z.JB, inputs, z.small)
        padding(z, c, k_ref, v_ref)

    each(T, normed_rows, z.small)

    def seen(base):
        slot = lax.broadcasted_iota(jnp.int32, (1, 128), 1) + base
        return ((slot % D) * T + slot // D < length) & (slot < N)

    for h in range(H):
        for t in range(T):
            span = pl.ds(t * D, D)
            line = t * H + h
            for n in range(z.full):
                keyed_ref[h, span, n * 128 : (n + 1) * 128] = raw_ref[pl.ds(n * T * H + line, D, stride=z.c2)]
            if z.rest:
                place, turned = line, False
                if z.pair:
                    group, groups = line // 8, T * H // 8
                    if group == groups - 1 and groups % 2:
                        place, turned = group // 2 * 8 + line % 4, line % 8 >= 4
                    else:
                        place, turned = group // 2 * 8 + line % 8, group % 2 == 1
                value = raw_ref[pl.ds(z.full * T * H + place, D, stride=z.c2)]
                keyed_ref[h, span, z.full * 128 :] = pltpu.roll(value, 64, 1) if turned else value
        scale = bound2[h : h + 1, 0:1]
        for a in range(z.NP // 128):
            for b in range(z.NP // 128):
                tile = keyed_ref[h, a * 128 : (a + 1) * 128, b * 128 : (b + 1) * 128].T
                plane_ref[h, b * 128 : (b + 1) * 128, a * 128 : (a + 1) * 128] = jnp.where(seen(a * 128), tile * scale, masked_score)

    def column(c):
        def block(b):
            span = at(b, z.JB)
            gated = (g_ref[c, span] * mixed(z, c, span, q_ref, k_ref, v_ref, plane_ref)).astype(bf16)
            g_ref[c, span] = jnp.dot(gated, out_w_ref[...], preferred_element_type=f32)

        each(N // z.JB, block, z.small)
        for t in range(T):
            pay_ref[pl.ds(t * T + c, D, stride=z.c3)] = g_ref[c, t * D : (t + 1) * D]

    each(T, column, z.small)

    @pl.loop(0, D // 2)
    def _(device):
        send_ref[at(device, 2 * z.c3)] = pay_ref[at(device, 2 * z.c3)].astype(bf16)


def last_kernel(z, recv_ref, middle_ref, out_ref, raw_ref, row_ref):
    T, D = z.T, z.D

    @pl.loop(0, D // 2)
    def _(device):
        raw_ref[at(device, 2 * z.c3)] = recv_ref[at(device, 2 * z.c3)].astype(f32)

    for t in range(T):
        for c in range(T):
            row_ref[t, pl.ds(c, D, stride=T)] = raw_ref[pl.ds(t * T + c, D, stride=z.c3)]
        out_ref[t] = (middle_ref[t].astype(f32) + row_ref[t]).astype(bf16)


def call(kernel, z, shapes, scratch, scalars, operands, flops, room=6 * 2**20, far=0, out=None, hbm=False):
    near = len(operands) - scalars - far
    specs = [pl.BlockSpec(memory_space=space) for space, count in ((pltpu.SMEM, scalars), (pltpu.VMEM, near), (pltpu.HBM, far)) for _ in range(count)]
    size = lambda shape, kind: math.prod(shape) * jnp.dtype(kind).itemsize
    moved = sum(size(a.shape, a.dtype) for a in operands) + sum(size(*result) for result in shapes)
    buffers = [entry for entry in scratch if isinstance(entry, tuple)]
    held = moved + sum(size(*entry) for entry in buffers)
    return pl.pallas_call(
        functools.partial(kernel, z),
        out_shape=[(pltpu.HBM if hbm else jax.ShapeDtypeStruct)(shape, kind) for shape, kind in shapes],
        in_specs=specs,
        out_specs=[pl.BlockSpec(memory_space=out or pltpu.VMEM)] * len(shapes),
        scratch_shapes=[pltpu.VMEM(*entry) if isinstance(entry, tuple) else entry for entry in scratch],
        cost_estimate=pl.CostEstimate(flops=flops, bytes_accessed=moved, transcendentals=0),
        compiler_params=pltpu.CompilerParams(vmem_limit_bytes=min(58 * 2**20, held + room)),
        name=kernel.__name__,
    )(*operands[: scalars + near], *(pltpu.with_memory_space_constraint(a, pltpu.HBM) for a in operands[scalars + near :]))


def exchange(values, z, rows):
    C = values.shape[-1]
    moved = lax.all_to_all(values.reshape(z.D, rows, C), both, split_axis=0, concat_axis=0, tiled=True)
    return moved.reshape(z.D * rows, C)


def shards(
    pair_tensor,
    lengths,
    starting_gain,
    starting_weights,
    starting_bias,
    starting_output,
    ending_gain,
    ending_weights,
    ending_bias,
    ending_output,
):
    H, R = lax.axis_size("heads"), lax.axis_size("rows")
    N, C = pair_tensor.shape[1:]
    z = Sizes(N, C, R, H)
    T, D, NP = z.T, z.D, z.NP
    i16 = jnp.int16
    gain1, gain2 = starting_gain.reshape(1, C), ending_gain.reshape(1, C)
    head = lax.axis_index("heads").astype(jnp.int32).reshape(1)

    dma = pltpu.SemaphoreType.DMA
    planes, packed, normed = call(
        first_plane_kernel, z,
        [((D * z.c1, C), i16), ((C + 16, C), bf16), ((T, N, C), bf16)],
        [
            ((z.L, N, C), bf16), ((N, z.L * C), bf16), ((z.L, NP), f32), ((2 * z.c1, C), i16), ((C + 16, C), bf16),
            ((1, C), f32), ((1, C), bf16), ((1, C), bf16),
            dma((z.L // 8,)), dma((T,)), dma((D // 2,)), dma((5,)),
        ],
        2, (head, lengths, gain1, starting_bias, ending_bias, starting_weights, pair_tensor),
        2 * z.L * N * C * 8, 58 * 2**20, far=5, out=pltpu.HBM, hbm=True,
    )
    planes = exchange(planes, z, z.c1)
    gathered = lax.all_gather(packed, "heads", axis=0, tiled=False)
    q, k, v, g, biases = call(
        project_kernel, z,
        [((T, H, N, C), bf16), ((T, NP, C), bf16), ((T, NP, C), bf16), ((T, N, C), f32), ((up(2 * H, 8), C), f32)],
        [((T, N, C), bf16), dma((1,))], 0, (gathered, normed), 2 * T * N * C * 7 * C, far=1,
    )
    middle, sent = call(
        first_node_kernel, z,
        [((T, N, C), bf16), ((D * z.c2, C), i16)],
        [((H, N, NP), f32), ((T, N, C), f32), ((N, T * C), bf16), ((T * H, NP), f32), ((D * z.c2, C), f32), ((T, N, C), bf16), ((T, N, C), bf16), ((D * z.c2, C), i16), dma((1,)), dma((5,))],
        2, (head, lengths, planes, q, k, v, g, biases, gain1, starting_output, gain2, pair_tensor), 4 * T * N * N * C * 2, far=1, out=pltpu.HBM, hbm=True,
    )
    received = exchange(sent, z, z.c2)
    ending_weights = lax.optimization_barrier((ending_weights, middle))[0]
    gathered = lax.all_gather(ending_weights, "heads", axis=0, tiled=False)
    (weights2,) = call(arrange_kernel, z, [((C, 7 * C), bf16)], [], 0, (gathered,), 4 * C * C)
    (sent,) = call(
        second_node_kernel, z,
        [((D * z.c3, C), bf16)],
        [
            ((D * z.c2, C), f32), ((T, N, C), bf16), ((T, H, N, C), bf16), ((T, NP, C), bf16), ((T, NP, C), bf16), ((T, N, C), f32),
            ((H, NP, NP), f32), ((H, NP, NP), f32), ((D * z.c3, C), f32),
        ],
        1, (lengths, received, weights2, biases, gain2, ending_output), 4 * T * N * N * C * 2,
    )
    received = exchange(sent, z, z.c3)
    (refined,) = call(
        last_kernel, z, [((T, N, C), bf16)], [((D * z.c3, C), f32), ((T, N, C), f32)], 0, (received, middle), T * N * C
    )
    return refined


def solution(mesh):
    placed = (
        P("rows", None, None),
        P(),
        P(),
        P(None, "heads"),
        P("heads", None),
        P(),
        P(),
        P(None, "heads"),
        P("heads", None),
        P(),
    )
    return jax.shard_map(
        shards,
        mesh=mesh,
        in_specs=placed,
        out_specs=P(both, None, None),
        check_vma=False,
    )
```

```python
import functools
import math

import jax
import jax.numpy as jnp
from jax import lax
from jax.experimental import pallas as pl
from jax.experimental.pallas import tpu as pltpu
from jax.sharding import PartitionSpec as P

epsilon = 1e-05
masked_score = -1e30
log2e = math.log2(math.e)
steps = 32767.0
fine = 262143.0
f32 = jnp.float32
bf16 = jnp.bfloat16
both = ("rows", "heads")


def up(value, multiple):
    return -(-value // multiple) * multiple


class Sizes:
    def __init__(self, tokens, channels, row_devices, heads):
        self.N, self.C, self.R, self.H = tokens, channels, row_devices, heads
        self.D = row_devices * heads
        self.L = tokens // row_devices
        self.T = tokens // self.D
        self.NP = up(tokens, 128)
        self.W = channels // heads
        self.full = tokens // 128
        self.rest = tokens % 128
        self.pair = self.rest == 64
        self.p1, self.c1 = self.planes(self.L)
        self.c1 = up(self.p1, 4)
        self.p2, self.c2 = self.planes(self.T * heads)
        self.low2 = up(self.p2 + self.T * self.T, 8)
        self.c2 = up(self.low2 + self.c2, 8)
        self.c3 = up(self.T * self.T, 4)
        self.small = tokens <= 256
        self.JB = tokens if self.small else 192

    def planes(self, rows):
        groups = rows // 8
        count = rows * self.full
        if self.pair:
            count += 8 * (groups // 2) + 4 * (groups % 2)
        elif self.rest:
            count += rows
        return count, 8 * (-(-(-(-count // 8)) // 5))


def each(count, body, unrolled=False):
    if count == 1 or unrolled:
        for index in range(count):
            body(index)
    else:

        @pl.loop(0, count)
        def _(index):
            body(index)


def at(index, size):
    if isinstance(index, int):
        return pl.ds(index * size, size)
    return pl.ds(pl.multiple_of(index * size, 8), size)


def nt(left, right):
    return lax.dot_general(left, right, (((1,), (1,)), ((), ())), preferred_element_type=f32)


def normalise(widened, gain):
    centre = jnp.mean(widened, axis=-1, keepdims=True)
    shifted = widened - centre
    spread = jnp.mean(shifted * shifted, axis=-1, keepdims=True)
    return (shifted * lax.rsqrt(spread + epsilon) * gain).astype(bf16)


def plane_bound(gain, bias, channels):
    product = gain * bias
    norm = jnp.sqrt(jnp.sum(product * product, axis=-1, keepdims=True))
    return jnp.maximum(norm * (1.01 * math.sqrt(channels)), 1e-20)


def normed_bound(gain, channels):
    return jnp.max(jnp.abs(gain), axis=-1, keepdims=True) * (1.01 * math.sqrt(channels))


def lanes(rows=8):
    return lax.broadcasted_iota(jnp.int32, (rows, 128), 1)


def sublanes():
    return lax.broadcasted_iota(jnp.int32, (8, 128), 0)


def plane_blocks(z, values):
    groups = values.shape[0] // 8
    blocks = [values[g * 8 : g * 8 + 8, n * 128 : n * 128 + 128] for n in range(z.full) for g in range(groups)]
    if z.rest:
        last = [values[g * 8 : g * 8 + 8, z.full * 128 :] for g in range(groups)]
        if z.pair:
            for g in range(0, groups - 1, 2):
                blocks.append(jnp.where(lanes() < 64, last[g], pltpu.roll(last[g + 1], 64, 1)))
            if groups % 2:
                blocks.append(jnp.where(lanes() < 64, last[-1], pltpu.roll(pltpu.roll(last[-1], 64, 1), 4, 0)))
        else:
            blocks += last
    return blocks


def digits(blocks):
    high, low = [], []
    for n, block in enumerate(blocks):
        whole = jnp.round(block).astype(jnp.int32)
        upper = (whole + 4) >> 3
        digit = (whole - upper * 8 + 4) << (3 * (n % 5))
        high.append(upper.astype(f32))
        low = low + [digit] if n % 5 == 0 else low[:-1] + [low[-1] + digit]
    return high, [block.astype(f32) for block in low]


def whole_value(high, low, number):
    return (high * 8 + ((low >> (3 * (number % 5))) & 7) - 4).astype(f32)


def log_scale(gain, bias, channels):
    return 65535.0 / jnp.log(1.0 + 2.0 * jnp.maximum(plane_bound(gain, bias, channels), 1e-3))


def first_plane_kernel(
    z, head_ref, lengths_ref, gain_far, bias_far, b2_far, w1_ref, pair_ref,
    out_ref, weights_ref, normed_ref, held_ref, wide_ref, plane_ref, copies_ref, pack_ref, gain_ref, bias_ref, b2_ref,
    arrived, left_sem, sent_sem, w_sem,
):
    N, C, L, T = z.N, z.C, z.L, z.T
    copies = [pltpu.make_async_copy(pair_ref.at[at(g, 8)], held_ref.at[at(g, 8)], arrived.at[g]) for g in range(L // 8)]
    small = ((gain_far, gain_ref), (bias_far, bias_ref), (b2_far, b2_ref), (w1_ref, pack_ref.at[pl.ds(0, C)]))
    small = [pltpu.make_async_copy(there, here, w_sem.at[n]) for n, (there, here) in enumerate(small)]
    for copy in small[:1] + copies + small[1:]:
        copy.start()
    small[0].wait()
    gain = gain_ref[...]
    for group in range(L // 8):
        copies[group].wait()
        for j in range(group * 8, group * 8 + 8):
            wide_ref[:, j * C : (j + 1) * C] = normalise(held_ref[j].astype(f32), gain)
    for copy in small[1:]:
        copy.wait()
    bias = bias_ref[...].astype(f32)
    row = lax.broadcasted_iota(jnp.int32, (16, C), 0)
    pack_ref[C : C + 16] = jnp.where(row == 0, bias, b2_ref[...].astype(f32)).astype(bf16)
    first = head_ref[0] * T
    sends = [pltpu.make_async_copy(pack_ref, weights_ref, w_sem.at[4])]
    for t in range(T):
        own = wide_ref.at[:, pl.ds(pl.multiple_of((first + t) * C, 128), C)]
        sends.append(pltpu.make_async_copy(own, normed_ref.at[t], left_sem.at[t]))
    for send in sends:
        send.start()

    row = lax.broadcasted_iota(jnp.int32, (L, C), 0)
    left = jnp.concatenate([jnp.where(row == j, bias, 0.0).astype(bf16) for j in range(L)], axis=1)
    plane_ref[:, 0:N] = nt(left, wide_ref[...])
    slot = lax.broadcasted_iota(jnp.int32, (L, z.NP), 1)
    plane = jnp.where((slot < lengths_ref[0]) & (slot < N), plane_ref[...], masked_score)
    below = jnp.max(plane, axis=-1, keepdims=True) - plane
    below = jnp.where(below < 1e20, below, 0.0)
    code = jnp.round(jnp.log(1.0 + below) * log_scale(gain, bias, C)) - 32768.0
    blocks = jnp.concatenate(plane_blocks(z, code), axis=0)[0 : z.c1].astype(jnp.int32)
    copies_ref[...] = jnp.concatenate([blocks] * 4, axis=0).astype(jnp.int16)
    for n in range(z.D // 4):
        sends.append(pltpu.make_async_copy(copies_ref, out_ref.at[at(n, 4 * z.c1)], sent_sem.at[n]))
        sends[-1].start()
    for send in sends:
        send.wait()


def arranged(z, columns):
    C, W, H = z.C, z.W, z.H
    lane = lax.broadcasted_iota(jnp.int32, (C, C), 1)
    own = [column.astype(f32) for column in columns]
    parts = []
    for kind in range(4):
        moved = [own[h] if h == kind else pltpu.roll(own[h], ((h - kind) * W) % C, 1) for h in range(H)]
        alone = [jnp.where((lane >= h * W) & (lane < (h + 1) * W), moved[h], 0.0) for h in range(H)]
        parts += [sum(alone[1:], alone[0])] if kind else alone
    return jnp.concatenate([part.astype(bf16) for part in parts], axis=1)


def project(z, normed, weights, t, span, q_ref, k_ref, v_ref, g_ref):
    C, H = z.C, z.H
    projected = jnp.dot(normed, weights, preferred_element_type=f32)
    part = lambda n: projected[:, n * C : (n + 1) * C]
    for h in range(H):
        q_ref[t, h, span] = part(h).astype(bf16)
    k_ref[t, span] = part(H).astype(bf16)
    v_ref[t, span] = part(H + 1).astype(bf16)
    g_ref[t, span] = 1.0 / (1.0 + jnp.exp(-part(H + 2)))


def padding(z, t, k_ref, v_ref):
    if z.NP > z.N:
        k_ref[t, z.N :] = jnp.zeros((z.NP - z.N, z.C), bf16)
        v_ref[t, z.N :] = jnp.zeros((z.NP - z.N, z.C), bf16)


def project_kernel(z, gathered_ref, normed_ref, q_ref, k_ref, v_ref, g_ref, bias_ref, held_ref, arrived):
    C = z.C
    copy = pltpu.make_async_copy(normed_ref, held_ref, arrived.at[0])
    copy.start()
    weights = arranged(z, [gathered_ref[h, 0:C] for h in range(z.H)])
    rows = [gathered_ref[h, C : C + 16].astype(f32) for h in range(z.H)]
    bias_ref[...] = jnp.zeros_like(bias_ref)
    for h in range(z.H):
        bias_ref[h : h + 1] = rows[h][0:1]
        bias_ref[z.H + h : z.H + h + 1] = rows[h][1:2]
    copy.wait()

    def row(t):
        def block(b):
            span = at(b, z.JB)
            project(z, held_ref[t, span], weights, t, span, q_ref, k_ref, v_ref, g_ref)

        each(z.N // z.JB, block, z.small)
        padding(z, t, k_ref, v_ref)

    each(z.T, row, z.small)


def arrange_kernel(z, gathered_ref, out_ref):
    out_ref[...] = arranged(z, [gathered_ref[h] for h in range(z.H)])


def attended(z, queries, keys, values, planes):
    rows = planes[0].shape[0]
    scores = nt(queries, keys) * (log2e / math.sqrt(z.W))
    parts = []
    for h in range(z.H):
        score = scores[h * rows : (h + 1) * rows] + planes[h]
        raised = jnp.exp2(score - jnp.max(score, axis=-1, keepdims=True))
        parts.append((raised * (1.0 / jnp.sum(raised, axis=-1, keepdims=True))).astype(bf16))
    sums = jnp.dot(jnp.concatenate(parts, axis=0), values, preferred_element_type=f32)
    lane = lax.broadcasted_iota(jnp.int32, (rows, z.C), 1)
    result = sums[(z.H - 1) * rows :]
    for h in range(z.H - 2, -1, -1):
        result = jnp.where(lane < (h + 1) * z.W, sums[h * rows : (h + 1) * rows], result)
    return result


def mixed(z, t, span, q_ref, k_ref, v_ref, plane_ref):
    queries = jnp.concatenate([q_ref[t, h, span] for h in range(z.H)], axis=0)
    return attended(z, queries, k_ref[t], v_ref[t], [plane_ref[h, span] for h in range(z.H)])


def first_node_kernel(
    z, head_ref, lengths_ref, recv_ref, q_ref, k_ref, v_ref, g_ref, bias_ref, gain1_ref, out_w_ref, gain2_ref, whole_ref,
    middle_out, send_out, plane_ref, row_ref, wide_ref, own_ref, pay_ref, pair_ref, middle_ref, send_ref, arrived, sent_sem,
):
    N, T, H, D, L, C = z.N, z.T, z.H, z.D, z.L, z.C
    length = lengths_ref[0]
    copy = pltpu.make_async_copy(whole_ref.at[pl.ds(head_ref[0] * T, T)], pair_ref, arrived.at[0])
    copy.start()
    unit = 1.0 / log_scale(gain1_ref[...], bias_ref[0:H], C)
    gain2 = gain2_ref[...]
    factor_n = steps / normed_bound(gain2, C)
    blocks = up(z.p1, 8) // 8
    groups = L // 8
    seen = [lanes() + n * 128 < length for n in range(z.full)]
    seen_rest = (lanes() + z.full * 128 < length) & (lanes() < z.rest)

    def decode(r):
        chunks = recv_ref[at(r, H * z.c1)].astype(jnp.int32)
        for h in range(H):
            chunk = chunks[h * z.c1 : (h + 1) * z.c1].astype(f32)
            value = (1.0 - jnp.exp((chunk + 32768.0) * unit[h : h + 1, 0:1])) * log2e
            value = jnp.concatenate([value, value[0 : blocks * 8 - z.c1]], axis=0) if z.c1 % 8 else value
            value = [value[n * 8 : n * 8 + 8] for n in range(blocks)]
            for g in range(groups):
                target = at(r * groups + g, 8)
                for n in range(z.full):
                    plane_ref[h, target, n * 128 : n * 128 + 128] = jnp.where(seen[n], value[n * groups + g], masked_score)
                if z.rest:
                    base = z.full * groups
                    if not z.pair:
                        last = value[base + g]
                    elif g == groups - 1 and g % 2 == 0:
                        last = value[base + g // 2]
                        last = jnp.where(sublanes() < 4, last, pltpu.roll(pltpu.roll(last, 64, 1), 4, 0))
                    else:
                        last = value[base + g // 2]
                        last = pltpu.roll(last, 64, 1) if g % 2 else last
                    plane_ref[h, target, z.full * 128 :] = jnp.where(seen_rest, last, masked_score)

    each(z.R, decode, z.small)
    if not z.small:
        copy.wait()
    def row(t):
        def block(b):
            span = at(b, z.JB)
            gated = (g_ref[t, span] * mixed(z, t, span, q_ref, k_ref, v_ref, plane_ref)).astype(bf16)
            if z.small and t == 0:
                copy.wait()
            update = jnp.dot(gated, out_w_ref[...], preferred_element_type=f32)
            middle = (pair_ref[t, span].astype(f32) + update).astype(bf16)
            middle_ref[t, span] = middle
            row_ref[t, span] = normalise(middle.astype(f32), gain2).astype(f32)

        each(N // z.JB, block, z.small)
        for c in range(T):
            piece = row_ref[t, pl.ds(c, D, stride=T)]
            lane = t * C if isinstance(t, int) else pl.multiple_of(t * C, 128)
            wide_ref[c * D : (c + 1) * D, pl.ds(lane, C)] = piece.astype(bf16)
            pay_ref[pl.ds(z.p2 + t * T + c, D, stride=z.c2)] = jnp.round(piece * factor_n)

    each(T, row, z.small)
    sends = [pltpu.make_async_copy(middle_ref, middle_out, sent_sem.at[0])]
    sends[0].start()
    bias2 = bias_ref[H : 2 * H]
    repeated = jnp.concatenate([bias2] * T, axis=0)
    line = lax.broadcasted_iota(jnp.int32, (T * H, C), 0)
    left = jnp.concatenate([jnp.where((line >= t * H) & (line < (t + 1) * H), repeated, 0.0).astype(bf16) for t in range(T)], axis=1)
    own_ref[:, 0:N] = nt(left, wide_ref[...]) * (fine / plane_bound(gain2, repeated, C))
    high, low = digits(plane_blocks(z, own_ref[...]))
    high = jnp.concatenate(high, axis=0)[0 : z.p2]
    low = jnp.concatenate(low, axis=0)

    share = D // 4
    for n in range(4):

        @pl.loop(n * share, (n + 1) * share, unroll=4)
        def _(device):
            pay_ref[pl.ds(pl.multiple_of(device * z.c2, 8), z.p2)] = high
            pay_ref[pl.ds(pl.multiple_of(device * z.c2 + z.low2, 8), low.shape[0])] = low

        @pl.loop(n * share // 2, (n + 1) * share // 2, unroll=2)
        def _(device):
            send_ref[at(device, 2 * z.c2)] = pay_ref[at(device, 2 * z.c2)].astype(jnp.int32).astype(jnp.int16)

        span = at(n, share * z.c2)
        sends.append(pltpu.make_async_copy(send_ref.at[span], send_out.at[span], sent_sem.at[1 + n]))
        sends[-1].start()
    for send in sends:
        send.wait()


def second_node_kernel(
    z, lengths_ref, recv_ref, w_ref, bias_ref, gain2_ref, out_w_ref,
    send_ref, raw_ref, column_ref, q_ref, k_ref, v_ref, g_ref, keyed_ref, plane_ref, pay_ref,
):
    N, T, H, D, C = z.N, z.T, z.H, z.D, z.C
    length = lengths_ref[0]
    gain2 = gain2_ref[...]
    bound2 = plane_bound(gain2, bias_ref[H : 2 * H], C) * (log2e / fine)
    scale_n = normed_bound(gain2, C) * (1.0 / steps)
    blocks = up(z.p2, 8) // 8

    @pl.loop(0, D // 2, unroll=2)
    def _(pair):
        both_chunks = recv_ref[at(pair, 2 * z.c2)].astype(jnp.int32)
        for half in range(2):
            chunk = both_chunks[half * z.c2 : (half + 1) * z.c2]
            start = pl.multiple_of(pair * (2 * z.c2) + half * z.c2, 8)
            for n in range(blocks):
                high = chunk[n * 8 : n * 8 + 8]
                value = whole_value(high, chunk[z.low2 + n // 5 * 8 : z.low2 + n // 5 * 8 + 8], n)
                if (n + 1) * 8 > z.p2:
                    value = jnp.where(sublanes() < z.p2 - n * 8, value, high.astype(f32))
                raw_ref[pl.ds(start + n * 8, 8)] = value
            raw_ref[pl.ds(start + blocks * 8, z.low2 - blocks * 8)] = chunk[blocks * 8 : z.low2].astype(f32)

    def normed_rows(c):
        for t in range(T):
            piece = raw_ref[pl.ds(z.p2 + t * T + c, D, stride=z.c2)]
            column_ref[c, t * D : (t + 1) * D] = (piece * scale_n).astype(bf16)

        def inputs(b):
            span = at(b, z.JB)
            project(z, column_ref[c, span], w_ref[...], c, span, q_ref, k_ref, v_ref, g_ref)

        each(N // z.JB, inputs, z.small)
        padding(z, c, k_ref, v_ref)

    each(T, normed_rows, z.small)

    def seen(base):
        slot = lax.broadcasted_iota(jnp.int32, (1, 128), 1) + base
        return ((slot % D) * T + slot // D < length) & (slot < N)

    for h in range(H):
        for t in range(T):
            span = pl.ds(t * D, D)
            line = t * H + h
            for n in range(z.full):
                keyed_ref[h, span, n * 128 : (n + 1) * 128] = raw_ref[pl.ds(n * T * H + line, D, stride=z.c2)]
            if z.rest:
                place, turned = line, False
                if z.pair:
                    group, groups = line // 8, T * H // 8
                    if group == groups - 1 and groups % 2:
                        place, turned = group // 2 * 8 + line % 4, line % 8 >= 4
                    else:
                        place, turned = group // 2 * 8 + line % 8, group % 2 == 1
                value = raw_ref[pl.ds(z.full * T * H + place, D, stride=z.c2)]
                keyed_ref[h, span, z.full * 128 :] = pltpu.roll(value, 64, 1) if turned else value
        scale = bound2[h : h + 1, 0:1]
        for a in range(z.NP // 128):
            for b in range(z.NP // 128):
                tile = keyed_ref[h, a * 128 : (a + 1) * 128, b * 128 : (b + 1) * 128].T
                plane_ref[h, b * 128 : (b + 1) * 128, a * 128 : (a + 1) * 128] = jnp.where(seen(a * 128), tile * scale, masked_score)

    def column(c):
        def block(b):
            span = at(b, z.JB)
            gated = (g_ref[c, span] * mixed(z, c, span, q_ref, k_ref, v_ref, plane_ref)).astype(bf16)
            g_ref[c, span] = jnp.dot(gated, out_w_ref[...], preferred_element_type=f32)

        each(N // z.JB, block, z.small)
        for t in range(T):
            pay_ref[pl.ds(t * T + c, D, stride=z.c3)] = g_ref[c, t * D : (t + 1) * D]

    each(T, column, z.small)

    @pl.loop(0, D // 4, unroll=2)
    def _(device):
        send_ref[at(device, 4 * z.c3)] = pay_ref[at(device, 4 * z.c3)].astype(bf16)


def last_kernel(z, recv_ref, middle_ref, out_ref, raw_ref, row_ref):
    T, D = z.T, z.D

    @pl.loop(0, D // 4, unroll=2)
    def _(device):
        raw_ref[at(device, 4 * z.c3)] = recv_ref[at(device, 4 * z.c3)].astype(f32)

    for t in range(T):
        for c in range(T):
            row_ref[t, pl.ds(c, D, stride=T)] = raw_ref[pl.ds(t * T + c, D, stride=z.c3)]
        out_ref[t] = (middle_ref[t].astype(f32) + row_ref[t]).astype(bf16)


def call(kernel, z, shapes, scratch, scalars, operands, flops, room=6 * 2**20, far=0, out=None, hbm=False):
    near = len(operands) - scalars - far
    specs = [pl.BlockSpec(memory_space=space) for space, count in ((pltpu.SMEM, scalars), (pltpu.VMEM, near), (pltpu.HBM, far)) for _ in range(count)]
    size = lambda shape, kind: math.prod(shape) * jnp.dtype(kind).itemsize
    moved = sum(size(a.shape, a.dtype) for a in operands) + sum(size(*result) for result in shapes)
    buffers = [entry for entry in scratch if isinstance(entry, tuple)]
    held = moved + sum(size(*entry) for entry in buffers)
    return pl.pallas_call(
        functools.partial(kernel, z),
        out_shape=[(pltpu.HBM if hbm else jax.ShapeDtypeStruct)(shape, kind) for shape, kind in shapes],
        in_specs=specs,
        out_specs=[pl.BlockSpec(memory_space=out or pltpu.VMEM)] * len(shapes),
        scratch_shapes=[pltpu.VMEM(*entry) if isinstance(entry, tuple) else entry for entry in scratch],
        cost_estimate=pl.CostEstimate(flops=flops, bytes_accessed=moved, transcendentals=0),
        compiler_params=pltpu.CompilerParams(vmem_limit_bytes=min(58 * 2**20, held + room)),
        name=kernel.__name__,
    )(*operands[: scalars + near], *(pltpu.with_memory_space_constraint(a, pltpu.HBM) for a in operands[scalars + near :]))


def exchange(values, z, rows):
    C = values.shape[-1]
    shape = (z.D, rows, C) if rows % 8 == 0 else (z.D, rows // 4, 4, C)
    moved = lax.all_to_all(values.reshape(shape), both, split_axis=0, concat_axis=0, tiled=True)
    return moved.reshape(z.D * rows, C)


def shards(
    pair_tensor,
    lengths,
    starting_gain,
    starting_weights,
    starting_bias,
    starting_output,
    ending_gain,
    ending_weights,
    ending_bias,
    ending_output,
):
    H, R = lax.axis_size("heads"), lax.axis_size("rows")
    N, C = pair_tensor.shape[1:]
    z = Sizes(N, C, R, H)
    T, D, NP = z.T, z.D, z.NP
    i16 = jnp.int16
    gain1, gain2 = starting_gain.reshape(1, C), ending_gain.reshape(1, C)
    head = lax.axis_index("heads").astype(jnp.int32).reshape(1)

    dma = pltpu.SemaphoreType.DMA
    planes, packed, normed = call(
        first_plane_kernel, z,
        [((D * z.c1, C), i16), ((C + 16, C), bf16), ((T, N, C), bf16)],
        [
            ((z.L, N, C), bf16), ((N, z.L * C), bf16), ((z.L, NP), f32), ((4 * z.c1, C), i16), ((C + 16, C), bf16),
            ((1, C), f32), ((1, C), bf16), ((1, C), bf16),
            dma((z.L // 8,)), dma((T,)), dma((D // 4,)), dma((5,)),
        ],
        2, (head, lengths, gain1, starting_bias, ending_bias, starting_weights, pair_tensor),
        2 * z.L * N * C * 8, 58 * 2**20, far=5, out=pltpu.HBM, hbm=True,
    )
    planes = exchange(planes, z, z.c1)
    gathered = lax.all_gather(packed, "heads", axis=0, tiled=False)
    q, k, v, g, biases = call(
        project_kernel, z,
        [((T, H, N, C), bf16), ((T, NP, C), bf16), ((T, NP, C), bf16), ((T, N, C), f32), ((up(2 * H, 8), C), f32)],
        [((T, N, C), bf16), dma((1,))], 0, (gathered, normed), 2 * T * N * C * 7 * C, far=1,
    )
    middle, sent = call(
        first_node_kernel, z,
        [((T, N, C), bf16), ((D * z.c2, C), i16)],
        [((H, N, NP), f32), ((T, N, C), f32), ((N, T * C), bf16), ((T * H, NP), f32), ((D * z.c2, C), f32), ((T, N, C), bf16), ((T, N, C), bf16), ((D * z.c2, C), i16), dma((1,)), dma((5,))],
        2, (head, lengths, planes, q, k, v, g, biases, gain1, starting_output, gain2, pair_tensor), 4 * T * N * N * C * 2, far=1, out=pltpu.HBM, hbm=True,
    )
    received = exchange(sent, z, z.c2)
    ending_weights = lax.optimization_barrier((ending_weights, middle))[0]
    gathered = lax.all_gather(ending_weights, "heads", axis=0, tiled=False)
    (weights2,) = call(arrange_kernel, z, [((C, 7 * C), bf16)], [], 0, (gathered,), 4 * C * C)
    (sent,) = call(
        second_node_kernel, z,
        [((D * z.c3, C), bf16)],
        [
            ((D * z.c2, C), f32), ((T, N, C), bf16), ((T, H, N, C), bf16), ((T, NP, C), bf16), ((T, NP, C), bf16), ((T, N, C), f32),
            ((H, NP, NP), f32), ((H, NP, NP), f32), ((D * z.c3, C), f32),
        ],
        1, (lengths, received, weights2, biases, gain2, ending_output), 4 * T * N * N * C * 2,
    )
    received = exchange(sent, z, z.c3)
    (refined,) = call(
        last_kernel, z, [((T, N, C), bf16)], [((D * z.c3, C), f32), ((T, N, C), f32)], 0, (received, middle), T * N * C
    )
    return refined


def solution(mesh):
    placed = (
        P("rows", None, None),
        P(),
        P(),
        P(None, "heads"),
        P("heads", None),
        P(),
        P(),
        P(None, "heads"),
        P("heads", None),
        P(),
    )
    return jax.shard_map(
        shards,
        mesh=mesh,
        in_specs=placed,
        out_specs=P(both, None, None),
        check_vma=False,
    )
```

```python
import functools
import math

import jax
import jax.numpy as jnp
from jax import lax
from jax.experimental import pallas as pl
from jax.experimental.pallas import tpu as pltpu
from jax.sharding import PartitionSpec as P

epsilon = 1e-05
masked_score = -1e30
log2e = math.log2(math.e)
steps = 32767.0
fine = 262143.0
f32 = jnp.float32
bf16 = jnp.bfloat16
both = ("rows", "heads")


def up(value, multiple):
    return -(-value // multiple) * multiple


class Sizes:
    def __init__(self, tokens, channels, row_devices, heads):
        self.N, self.C, self.R, self.H = tokens, channels, row_devices, heads
        self.D = row_devices * heads
        self.L = tokens // row_devices
        self.T = tokens // self.D
        self.NP = up(tokens, 128)
        self.W = channels // heads
        self.full = tokens // 128
        self.rest = tokens % 128
        self.pair = self.rest == 64
        self.p1, self.c1 = self.planes(self.L)
        self.c1 = up(self.p1, 4)
        self.p2, self.c2 = self.planes(self.T * heads)
        self.low2 = up(self.p2 + self.T * self.T, 8)
        self.c2 = up(self.low2 + self.c2, 8)
        self.c3 = up(self.T * self.T, 4)
        self.small = tokens <= 256
        self.JB = tokens if self.small else 192

    def planes(self, rows):
        groups = rows // 8
        count = rows * self.full
        if self.pair:
            count += 8 * (groups // 2) + 4 * (groups % 2)
        elif self.rest:
            count += rows
        return count, 8 * (-(-(-(-count // 8)) // 5))


def each(count, body, unrolled=False):
    if count == 1 or unrolled:
        for index in range(count):
            body(index)
    else:

        @pl.loop(0, count)
        def _(index):
            body(index)


def at(index, size):
    if isinstance(index, int):
        return pl.ds(index * size, size)
    return pl.ds(pl.multiple_of(index * size, 8), size)


def nt(left, right):
    return lax.dot_general(left, right, (((1,), (1,)), ((), ())), preferred_element_type=f32)


def normalise(values, gain, multiplied=False):
    C = values.shape[-1]
    widened = values.astype(f32)
    if multiplied and C & (C - 1) == 0:
        centre = jnp.dot(values, jnp.full((C, C), 1.0 / C, bf16), preferred_element_type=f32)
    else:
        centre = jnp.mean(widened, axis=-1, keepdims=True)
    shifted = widened - centre
    spread = jnp.mean(shifted * shifted, axis=-1, keepdims=True)
    return (shifted * lax.rsqrt(spread + epsilon) * gain).astype(bf16)


def plane_bound(gain, bias, channels):
    product = gain * bias
    norm = jnp.sqrt(jnp.sum(product * product, axis=-1, keepdims=True))
    return jnp.maximum(norm * (1.01 * math.sqrt(channels)), 1e-20)


def normed_bound(gain, channels):
    return jnp.max(jnp.abs(gain), axis=-1, keepdims=True) * (1.01 * math.sqrt(channels))


def lanes(rows=8):
    return lax.broadcasted_iota(jnp.int32, (rows, 128), 1)


def sublanes():
    return lax.broadcasted_iota(jnp.int32, (8, 128), 0)


def plane_blocks(z, values):
    groups = values.shape[0] // 8
    blocks = [values[g * 8 : g * 8 + 8, n * 128 : n * 128 + 128] for n in range(z.full) for g in range(groups)]
    if z.rest:
        last = [values[g * 8 : g * 8 + 8, z.full * 128 :] for g in range(groups)]
        if z.pair:
            for g in range(0, groups - 1, 2):
                blocks.append(jnp.where(lanes() < 64, last[g], pltpu.roll(last[g + 1], 64, 1)))
            if groups % 2:
                blocks.append(jnp.where(lanes() < 64, last[-1], pltpu.roll(pltpu.roll(last[-1], 64, 1), 4, 0)))
        else:
            blocks += last
    return blocks


def digits(blocks):
    high, low = [], []
    for n, block in enumerate(blocks):
        whole = jnp.round(block).astype(jnp.int32)
        upper = (whole + 4) >> 3
        digit = (whole - upper * 8 + 4) << (3 * (n % 5))
        high.append(upper.astype(f32))
        low = low + [digit] if n % 5 == 0 else low[:-1] + [low[-1] + digit]
    return high, [block.astype(f32) for block in low]


def whole_value(high, low, number):
    return (high * 8 + ((low >> (3 * (number % 5))) & 7) - 4).astype(f32)


def log_scale(gain, bias, channels):
    return 65535.0 / jnp.log(1.0 + 2.0 * jnp.maximum(plane_bound(gain, bias, channels), 1e-3))


def first_plane_kernel(
    z, head_ref, lengths_ref, gain_far, bias_far, b2_far, w1_ref, pair_ref,
    out_ref, weights_ref, normed_ref, held_ref, wide_ref, plane_ref, copies_ref, pack_ref, gain_ref, bias_ref, b2_ref,
    arrived, left_sem, sent_sem, w_sem,
):
    N, C, L, T = z.N, z.C, z.L, z.T
    copies = [pltpu.make_async_copy(pair_ref.at[at(g, 8)], held_ref.at[at(g, 8)], arrived.at[g]) for g in range(L // 8)]
    small = ((gain_far, gain_ref), (bias_far, bias_ref), (b2_far, b2_ref), (w1_ref, pack_ref.at[pl.ds(0, C)]))
    small = [pltpu.make_async_copy(there, here, w_sem.at[n]) for n, (there, here) in enumerate(small)]
    for copy in small[:1] + copies + small[1:]:
        copy.start()
    small[0].wait()
    gain = gain_ref[...]
    for group in range(L // 8):
        copies[group].wait()
        for j in range(group * 8, group * 8 + 8):
            wide_ref[:, j * C : (j + 1) * C] = normalise(held_ref[j], gain, True)
    for copy in small[1:]:
        copy.wait()
    bias = bias_ref[...].astype(f32)
    row = lax.broadcasted_iota(jnp.int32, (16, C), 0)
    pack_ref[C : C + 16] = jnp.where(row == 0, bias, b2_ref[...].astype(f32)).astype(bf16)
    first = head_ref[0] * T
    sends = [pltpu.make_async_copy(pack_ref, weights_ref, w_sem.at[4])]
    for t in range(T):
        own = wide_ref.at[:, pl.ds(pl.multiple_of((first + t) * C, 128), C)]
        sends.append(pltpu.make_async_copy(own, normed_ref.at[t], left_sem.at[t]))
    for send in sends:
        send.start()

    row = lax.broadcasted_iota(jnp.int32, (L, C), 0)
    left = jnp.concatenate([jnp.where(row == j, bias, 0.0).astype(bf16) for j in range(L)], axis=1)
    plane_ref[:, 0:N] = nt(left, wide_ref[...])
    slot = lax.broadcasted_iota(jnp.int32, (L, z.NP), 1)
    plane = jnp.where((slot < lengths_ref[0]) & (slot < N), plane_ref[...], masked_score)
    below = jnp.max(plane, axis=-1, keepdims=True) - plane
    below = jnp.where(below < 1e20, below, 0.0)
    code = jnp.round(jnp.log(1.0 + below) * log_scale(gain, bias, C)) - 32768.0
    blocks = jnp.concatenate(plane_blocks(z, code), axis=0)[0 : z.c1].astype(jnp.int32)
    copies_ref[...] = jnp.concatenate([blocks] * 4, axis=0).astype(jnp.int16)
    for n in range(z.D // 4):
        sends.append(pltpu.make_async_copy(copies_ref, out_ref.at[at(n, 4 * z.c1)], sent_sem.at[n]))
        sends[-1].start()
    for send in sends:
        send.wait()


def arranged(z, columns):
    C, W, H = z.C, z.W, z.H
    lane = lax.broadcasted_iota(jnp.int32, (C, C), 1)
    own = [column.astype(f32) for column in columns]
    parts = []
    for kind in range(4):
        moved = [own[h] if h == kind else pltpu.roll(own[h], ((h - kind) * W) % C, 1) for h in range(H)]
        alone = [jnp.where((lane >= h * W) & (lane < (h + 1) * W), moved[h], 0.0) for h in range(H)]
        parts += [sum(alone[1:], alone[0])] if kind else alone
    return jnp.concatenate([part.astype(bf16) for part in parts], axis=1)


def project(z, normed, weights, t, span, q_ref, k_ref, v_ref, g_ref):
    C, H = z.C, z.H
    projected = jnp.dot(normed, weights, preferred_element_type=f32)
    part = lambda n: projected[:, n * C : (n + 1) * C]
    for h in range(H):
        q_ref[t, h, span] = part(h).astype(bf16)
    k_ref[t, span] = part(H).astype(bf16)
    v_ref[t, span] = part(H + 1).astype(bf16)
    g_ref[t, span] = 1.0 / (1.0 + jnp.exp(-part(H + 2)))


def padding(z, t, k_ref, v_ref):
    if z.NP > z.N:
        k_ref[t, z.N :] = jnp.zeros((z.NP - z.N, z.C), bf16)
        v_ref[t, z.N :] = jnp.zeros((z.NP - z.N, z.C), bf16)


def project_kernel(z, gathered_ref, normed_ref, q_ref, k_ref, v_ref, g_ref, bias_ref, held_ref, arrived):
    C = z.C
    copy = pltpu.make_async_copy(normed_ref, held_ref, arrived.at[0])
    copy.start()
    weights = arranged(z, [gathered_ref[h, 0:C] for h in range(z.H)])
    rows = [gathered_ref[h, C : C + 16].astype(f32) for h in range(z.H)]
    bias_ref[...] = jnp.zeros_like(bias_ref)
    for h in range(z.H):
        bias_ref[h : h + 1] = rows[h][0:1]
        bias_ref[z.H + h : z.H + h + 1] = rows[h][1:2]
    copy.wait()

    def row(t):
        def block(b):
            span = at(b, z.JB)
            project(z, held_ref[t, span], weights, t, span, q_ref, k_ref, v_ref, g_ref)

        each(z.N // z.JB, block, z.small)
        padding(z, t, k_ref, v_ref)

    each(z.T, row, z.small)


def arrange_kernel(z, gathered_ref, out_ref):
    out_ref[...] = arranged(z, [gathered_ref[h] for h in range(z.H)])


def attended(z, queries, keys, values, planes):
    rows = planes[0].shape[0]
    scores = nt(queries, keys) * (log2e / math.sqrt(z.W))
    parts = []
    for h in range(z.H):
        score = scores[h * rows : (h + 1) * rows] + planes[h]
        raised = jnp.exp2(score - jnp.max(score, axis=-1, keepdims=True))
        parts.append((raised * (1.0 / jnp.sum(raised, axis=-1, keepdims=True))).astype(bf16))
    sums = jnp.dot(jnp.concatenate(parts, axis=0), values, preferred_element_type=f32)
    lane = lax.broadcasted_iota(jnp.int32, (rows, z.C), 1)
    result = sums[(z.H - 1) * rows :]
    for h in range(z.H - 2, -1, -1):
        result = jnp.where(lane < (h + 1) * z.W, sums[h * rows : (h + 1) * rows], result)
    return result


def mixed(z, t, span, q_ref, k_ref, v_ref, plane_ref):
    queries = jnp.concatenate([q_ref[t, h, span] for h in range(z.H)], axis=0)
    return attended(z, queries, k_ref[t], v_ref[t], [plane_ref[h, span] for h in range(z.H)])


def first_node_kernel(
    z, head_ref, lengths_ref, recv_ref, q_ref, k_ref, v_ref, g_ref, bias_ref, gain1_ref, out_w_ref, gain2_ref, whole_ref,
    middle_out, send_out, plane_ref, row_ref, wide_ref, own_ref, pay_ref, pair_ref, middle_ref, send_ref, arrived, sent_sem,
):
    N, T, H, D, L, C = z.N, z.T, z.H, z.D, z.L, z.C
    length = lengths_ref[0]
    copy = pltpu.make_async_copy(whole_ref.at[pl.ds(head_ref[0] * T, T)], pair_ref, arrived.at[0])
    copy.start()
    unit = 1.0 / log_scale(gain1_ref[...], bias_ref[0:H], C)
    gain2 = gain2_ref[...]
    factor_n = steps / normed_bound(gain2, C)
    blocks = up(z.p1, 8) // 8
    groups = L // 8
    seen = [lanes() + n * 128 < length for n in range(z.full)]
    seen_rest = (lanes() + z.full * 128 < length) & (lanes() < z.rest)

    def decode(r):
        chunks = recv_ref[at(r, H * z.c1)].astype(jnp.int32)
        for h in range(H):
            chunk = chunks[h * z.c1 : (h + 1) * z.c1].astype(f32)
            value = (1.0 - jnp.exp((chunk + 32768.0) * unit[h : h + 1, 0:1])) * log2e
            value = jnp.concatenate([value, value[0 : blocks * 8 - z.c1]], axis=0) if z.c1 % 8 else value
            value = [value[n * 8 : n * 8 + 8] for n in range(blocks)]
            for g in range(groups):
                target = at(r * groups + g, 8)
                for n in range(z.full):
                    plane_ref[h, target, n * 128 : n * 128 + 128] = jnp.where(seen[n], value[n * groups + g], masked_score)
                if z.rest:
                    base = z.full * groups
                    if not z.pair:
                        last = value[base + g]
                    elif g == groups - 1 and g % 2 == 0:
                        last = value[base + g // 2]
                        last = jnp.where(sublanes() < 4, last, pltpu.roll(pltpu.roll(last, 64, 1), 4, 0))
                    else:
                        last = value[base + g // 2]
                        last = pltpu.roll(last, 64, 1) if g % 2 else last
                    plane_ref[h, target, z.full * 128 :] = jnp.where(seen_rest, last, masked_score)

    each(z.R, decode, z.small)
    if not z.small:
        copy.wait()
    def row(t):
        def block(b):
            span = at(b, z.JB)
            gated = (g_ref[t, span] * mixed(z, t, span, q_ref, k_ref, v_ref, plane_ref)).astype(bf16)
            if z.small and t == 0:
                copy.wait()
            update = jnp.dot(gated, out_w_ref[...], preferred_element_type=f32)
            middle = (pair_ref[t, span].astype(f32) + update).astype(bf16)
            middle_ref[t, span] = middle
            row_ref[t, span] = normalise(middle, gain2).astype(f32)

        each(N // z.JB, block, z.small)
        for c in range(T):
            piece = row_ref[t, pl.ds(c, D, stride=T)]
            lane = t * C if isinstance(t, int) else pl.multiple_of(t * C, 128)
            wide_ref[c * D : (c + 1) * D, pl.ds(lane, C)] = piece.astype(bf16)
            pay_ref[pl.ds(z.p2 + t * T + c, D, stride=z.c2)] = jnp.round(piece * factor_n)

    each(T, row, z.small)
    sends = [pltpu.make_async_copy(middle_ref, middle_out, sent_sem.at[0])]
    sends[0].start()
    bias2 = bias_ref[H : 2 * H]
    repeated = jnp.concatenate([bias2] * T, axis=0)
    line = lax.broadcasted_iota(jnp.int32, (T * H, C), 0)
    left = jnp.concatenate([jnp.where((line >= t * H) & (line < (t + 1) * H), repeated, 0.0).astype(bf16) for t in range(T)], axis=1)
    own_ref[:, 0:N] = nt(left, wide_ref[...]) * (fine / plane_bound(gain2, repeated, C))
    high, low = digits(plane_blocks(z, own_ref[...]))
    high = jnp.concatenate(high, axis=0)[0 : z.p2]
    low = jnp.concatenate(low, axis=0)

    share = D // 4
    for n in range(4):

        @pl.loop(n * share, (n + 1) * share, unroll=4)
        def _(device):
            pay_ref[pl.ds(pl.multiple_of(device * z.c2, 8), z.p2)] = high
            pay_ref[pl.ds(pl.multiple_of(device * z.c2 + z.low2, 8), low.shape[0])] = low

        @pl.loop(n * share // 2, (n + 1) * share // 2, unroll=2)
        def _(device):
            send_ref[at(device, 2 * z.c2)] = pay_ref[at(device, 2 * z.c2)].astype(jnp.int32).astype(jnp.int16)

        span = at(n, share * z.c2)
        sends.append(pltpu.make_async_copy(send_ref.at[span], send_out.at[span], sent_sem.at[1 + n]))
        sends[-1].start()
    for send in sends:
        send.wait()


def second_node_kernel(
    z, lengths_ref, recv_ref, w_ref, bias_ref, gain2_ref, out_w_ref,
    send_ref, raw_ref, column_ref, q_ref, k_ref, v_ref, g_ref, keyed_ref, plane_ref, pay_ref,
):
    N, T, H, D, C = z.N, z.T, z.H, z.D, z.C
    length = lengths_ref[0]
    gain2 = gain2_ref[...]
    bound2 = plane_bound(gain2, bias_ref[H : 2 * H], C) * (log2e / fine)
    scale_n = normed_bound(gain2, C) * (1.0 / steps)
    blocks = up(z.p2, 8) // 8

    @pl.loop(0, D // 2, unroll=2)
    def _(pair):
        both_chunks = recv_ref[at(pair, 2 * z.c2)].astype(jnp.int32)
        for half in range(2):
            chunk = both_chunks[half * z.c2 : (half + 1) * z.c2]
            start = pl.multiple_of(pair * (2 * z.c2) + half * z.c2, 8)
            for n in range(blocks):
                high = chunk[n * 8 : n * 8 + 8]
                value = whole_value(high, chunk[z.low2 + n // 5 * 8 : z.low2 + n // 5 * 8 + 8], n)
                if (n + 1) * 8 > z.p2:
                    value = jnp.where(sublanes() < z.p2 - n * 8, value, high.astype(f32))
                raw_ref[pl.ds(start + n * 8, 8)] = value
            raw_ref[pl.ds(start + blocks * 8, z.low2 - blocks * 8)] = chunk[blocks * 8 : z.low2].astype(f32)

    def normed_rows(c):
        for t in range(T):
            piece = raw_ref[pl.ds(z.p2 + t * T + c, D, stride=z.c2)]
            column_ref[c, t * D : (t + 1) * D] = (piece * scale_n).astype(bf16)

        def inputs(b):
            span = at(b, z.JB)
            project(z, column_ref[c, span], w_ref[...], c, span, q_ref, k_ref, v_ref, g_ref)

        each(N // z.JB, inputs, z.small)
        padding(z, c, k_ref, v_ref)

    each(T, normed_rows, z.small)

    def seen(base):
        slot = lax.broadcasted_iota(jnp.int32, (1, 128), 1) + base
        return ((slot % D) * T + slot // D < length) & (slot < N)

    for h in range(H):
        for t in range(T):
            span = pl.ds(t * D, D)
            line = t * H + h
            for n in range(z.full):
                keyed_ref[h, span, n * 128 : (n + 1) * 128] = raw_ref[pl.ds(n * T * H + line, D, stride=z.c2)]
            if z.rest:
                place, turned = line, False
                if z.pair:
                    group, groups = line // 8, T * H // 8
                    if group == groups - 1 and groups % 2:
                        place, turned = group // 2 * 8 + line % 4, line % 8 >= 4
                    else:
                        place, turned = group // 2 * 8 + line % 8, group % 2 == 1
                value = raw_ref[pl.ds(z.full * T * H + place, D, stride=z.c2)]
                keyed_ref[h, span, z.full * 128 :] = pltpu.roll(value, 64, 1) if turned else value
        scale = bound2[h : h + 1, 0:1]
        for a in range(z.NP // 128):
            for b in range(z.NP // 128):
                tile = keyed_ref[h, a * 128 : (a + 1) * 128, b * 128 : (b + 1) * 128].T
                plane_ref[h, b * 128 : (b + 1) * 128, a * 128 : (a + 1) * 128] = jnp.where(seen(a * 128), tile * scale, masked_score)

    def column(c):
        def block(b):
            span = at(b, z.JB)
            gated = (g_ref[c, span] * mixed(z, c, span, q_ref, k_ref, v_ref, plane_ref)).astype(bf16)
            g_ref[c, span] = jnp.dot(gated, out_w_ref[...], preferred_element_type=f32)

        each(N // z.JB, block, z.small)
        for t in range(T):
            pay_ref[pl.ds(t * T + c, D, stride=z.c3)] = g_ref[c, t * D : (t + 1) * D]

    each(T, column, z.small)

    @pl.loop(0, D // 4, unroll=2)
    def _(device):
        send_ref[at(device, 4 * z.c3)] = pay_ref[at(device, 4 * z.c3)].astype(bf16)


def last_kernel(z, recv_ref, middle_ref, out_ref, raw_ref, row_ref):
    T, D = z.T, z.D

    @pl.loop(0, D // 4, unroll=2)
    def _(device):
        raw_ref[at(device, 4 * z.c3)] = recv_ref[at(device, 4 * z.c3)].astype(f32)

    for t in range(T):
        for c in range(T):
            row_ref[t, pl.ds(c, D, stride=T)] = raw_ref[pl.ds(t * T + c, D, stride=z.c3)]
        out_ref[t] = (middle_ref[t].astype(f32) + row_ref[t]).astype(bf16)


def call(kernel, z, shapes, scratch, scalars, operands, flops, room=6 * 2**20, far=0, out=None, hbm=False):
    near = len(operands) - scalars - far
    specs = [pl.BlockSpec(memory_space=space) for space, count in ((pltpu.SMEM, scalars), (pltpu.VMEM, near), (pltpu.HBM, far)) for _ in range(count)]
    size = lambda shape, kind: math.prod(shape) * jnp.dtype(kind).itemsize
    moved = sum(size(a.shape, a.dtype) for a in operands) + sum(size(*result) for result in shapes)
    buffers = [entry for entry in scratch if isinstance(entry, tuple)]
    held = moved + sum(size(*entry) for entry in buffers)
    return pl.pallas_call(
        functools.partial(kernel, z),
        out_shape=[(pltpu.HBM if hbm else jax.ShapeDtypeStruct)(shape, kind) for shape, kind in shapes],
        in_specs=specs,
        out_specs=[pl.BlockSpec(memory_space=out or pltpu.VMEM)] * len(shapes),
        scratch_shapes=[pltpu.VMEM(*entry) if isinstance(entry, tuple) else entry for entry in scratch],
        cost_estimate=pl.CostEstimate(flops=flops, bytes_accessed=moved, transcendentals=0),
        compiler_params=pltpu.CompilerParams(vmem_limit_bytes=min(58 * 2**20, held + room)),
        name=kernel.__name__,
    )(*operands[: scalars + near], *(pltpu.with_memory_space_constraint(a, pltpu.HBM) for a in operands[scalars + near :]))


def exchange(values, z, rows):
    C = values.shape[-1]
    shape = (z.D, rows, C) if rows % 8 == 0 else (z.D, rows // 4, 4, C)
    moved = lax.all_to_all(values.reshape(shape), both, split_axis=0, concat_axis=0, tiled=True)
    return moved.reshape(z.D * rows, C)


def shards(
    pair_tensor,
    lengths,
    starting_gain,
    starting_weights,
    starting_bias,
    starting_output,
    ending_gain,
    ending_weights,
    ending_bias,
    ending_output,
):
    H, R = lax.axis_size("heads"), lax.axis_size("rows")
    N, C = pair_tensor.shape[1:]
    z = Sizes(N, C, R, H)
    T, D, NP = z.T, z.D, z.NP
    i16 = jnp.int16
    gain1, gain2 = starting_gain.reshape(1, C), ending_gain.reshape(1, C)
    head = lax.axis_index("heads").astype(jnp.int32).reshape(1)

    dma = pltpu.SemaphoreType.DMA
    planes, packed, normed = call(
        first_plane_kernel, z,
        [((D * z.c1, C), i16), ((C + 16, C), bf16), ((T, N, C), bf16)],
        [
            ((z.L, N, C), bf16), ((N, z.L * C), bf16), ((z.L, NP), f32), ((4 * z.c1, C), i16), ((C + 16, C), bf16),
            ((1, C), f32), ((1, C), bf16), ((1, C), bf16),
            dma((z.L // 8,)), dma((T,)), dma((D // 4,)), dma((5,)),
        ],
        2, (head, lengths, gain1, starting_bias, ending_bias, starting_weights, pair_tensor),
        2 * z.L * N * C * 8, 58 * 2**20, far=5, out=pltpu.HBM, hbm=True,
    )
    planes = exchange(planes, z, z.c1)
    gathered = lax.all_gather(packed, "heads", axis=0, tiled=False)
    q, k, v, g, biases = call(
        project_kernel, z,
        [((T, H, N, C), bf16), ((T, NP, C), bf16), ((T, NP, C), bf16), ((T, N, C), f32), ((up(2 * H, 8), C), f32)],
        [((T, N, C), bf16), dma((1,))], 0, (gathered, normed), 2 * T * N * C * 7 * C, far=1,
    )
    middle, sent = call(
        first_node_kernel, z,
        [((T, N, C), bf16), ((D * z.c2, C), i16)],
        [((H, N, NP), f32), ((T, N, C), f32), ((N, T * C), bf16), ((T * H, NP), f32), ((D * z.c2, C), f32), ((T, N, C), bf16), ((T, N, C), bf16), ((D * z.c2, C), i16), dma((1,)), dma((5,))],
        2, (head, lengths, planes, q, k, v, g, biases, gain1, starting_output, gain2, pair_tensor), 4 * T * N * N * C * 2, far=1, out=pltpu.HBM, hbm=True,
    )
    received = exchange(sent, z, z.c2)
    ending_weights = lax.optimization_barrier((ending_weights, middle))[0]
    gathered = lax.all_gather(ending_weights, "heads", axis=0, tiled=False)
    (weights2,) = call(arrange_kernel, z, [((C, 7 * C), bf16)], [], 0, (gathered,), 4 * C * C)
    (sent,) = call(
        second_node_kernel, z,
        [((D * z.c3, C), bf16)],
        [
            ((D * z.c2, C), f32), ((T, N, C), bf16), ((T, H, N, C), bf16), ((T, NP, C), bf16), ((T, NP, C), bf16), ((T, N, C), f32),
            ((H, NP, NP), f32), ((H, NP, NP), f32), ((D * z.c3, C), f32),
        ],
        1, (lengths, received, weights2, biases, gain2, ending_output), 4 * T * N * N * C * 2,
    )
    received = exchange(sent, z, z.c3)
    (refined,) = call(
        last_kernel, z, [((T, N, C), bf16)], [((D * z.c3, C), f32), ((T, N, C), f32)], 0, (received, middle), T * N * C
    )
    return refined


def solution(mesh):
    placed = (
        P("rows", None, None),
        P(),
        P(),
        P(None, "heads"),
        P("heads", None),
        P(),
        P(),
        P(None, "heads"),
        P("heads", None),
        P(),
    )
    return jax.shard_map(
        shards,
        mesh=mesh,
        in_specs=placed,
        out_specs=P(both, None, None),
        check_vma=False,
    )
```

```python
import functools
import math

import jax
import jax.numpy as jnp
from jax import lax
from jax.experimental import pallas as pl
from jax.experimental.pallas import tpu as pltpu
from jax.sharding import PartitionSpec as P

epsilon = 1e-05
masked_score = -1e30
log2e = math.log2(math.e)
steps = 32767.0
fine = 262143.0
f32 = jnp.float32
bf16 = jnp.bfloat16
both = ("rows", "heads")


def up(value, multiple):
    return -(-value // multiple) * multiple


class Sizes:
    def __init__(self, tokens, channels, row_devices, heads):
        self.N, self.C, self.R, self.H = tokens, channels, row_devices, heads
        self.D = row_devices * heads
        self.L = tokens // row_devices
        self.T = tokens // self.D
        self.NP = up(tokens, 128)
        self.W = channels // heads
        self.full = tokens // 128
        self.rest = tokens % 128
        self.pair = self.rest == 64
        self.p1, self.c1 = self.planes(self.L)
        self.c1 = up(self.p1, 4)
        self.p2, self.c2 = self.planes(self.T * heads)
        self.low2 = up(self.p2 + self.T * self.T, 8)
        self.c2 = up(self.low2 + self.c2, 8)
        self.c3 = up(self.T * self.T, 4)
        self.small = tokens <= 256
        self.JB = tokens if self.small else 192

    def planes(self, rows):
        groups = rows // 8
        count = rows * self.full
        if self.pair:
            count += 8 * (groups // 2) + 4 * (groups % 2)
        elif self.rest:
            count += rows
        return count, 8 * (-(-(-(-count // 8)) // 5))


def each(count, body, unrolled=False):
    if count == 1 or unrolled:
        for index in range(count):
            body(index)
    else:

        @pl.loop(0, count)
        def _(index):
            body(index)


def at(index, size):
    if isinstance(index, int):
        return pl.ds(index * size, size)
    return pl.ds(pl.multiple_of(index * size, 8), size)


def nt(left, right):
    return lax.dot_general(left, right, (((1,), (1,)), ((), ())), preferred_element_type=f32)


def normalise(values, gain, multiplied=False):
    C = values.shape[-1]
    widened = values.astype(f32)
    if multiplied and C & (C - 1) == 0:
        centre = jnp.dot(values, jnp.full((C, C), 1.0 / C, bf16), preferred_element_type=f32)
    else:
        centre = jnp.mean(widened, axis=-1, keepdims=True)
    shifted = widened - centre
    spread = jnp.mean(shifted * shifted, axis=-1, keepdims=True)
    return (shifted * lax.rsqrt(spread + epsilon) * gain).astype(bf16)


def plane_bound(gain, bias, channels):
    product = gain * bias
    norm = jnp.sqrt(jnp.sum(product * product, axis=-1, keepdims=True))
    return jnp.maximum(norm * (1.01 * math.sqrt(channels)), 1e-20)


def normed_bound(gain, channels):
    return jnp.max(jnp.abs(gain), axis=-1, keepdims=True) * (1.01 * math.sqrt(channels))


def lanes(rows=8):
    return lax.broadcasted_iota(jnp.int32, (rows, 128), 1)


def sublanes():
    return lax.broadcasted_iota(jnp.int32, (8, 128), 0)


def plane_blocks(z, values):
    groups = values.shape[0] // 8
    blocks = [values[g * 8 : g * 8 + 8, n * 128 : n * 128 + 128] for n in range(z.full) for g in range(groups)]
    if z.rest:
        last = [values[g * 8 : g * 8 + 8, z.full * 128 :] for g in range(groups)]
        if z.pair:
            for g in range(0, groups - 1, 2):
                blocks.append(jnp.where(lanes() < 64, last[g], pltpu.roll(last[g + 1], 64, 1)))
            if groups % 2:
                blocks.append(jnp.where(lanes() < 64, last[-1], pltpu.roll(pltpu.roll(last[-1], 64, 1), 4, 0)))
        else:
            blocks += last
    return blocks


def digits(blocks):
    high, low = [], []
    for n, block in enumerate(blocks):
        whole = jnp.round(block).astype(jnp.int32)
        upper = (whole + 4) >> 3
        digit = (whole - upper * 8 + 4) << (3 * (n % 5))
        high.append(upper.astype(f32))
        low = low + [digit] if n % 5 == 0 else low[:-1] + [low[-1] + digit]
    return high, [block.astype(f32) for block in low]


def whole_value(high, low, number):
    return (high * 8 + ((low >> (3 * (number % 5))) & 7) - 4).astype(f32)


def log_scale(gain, bias, channels):
    return 65535.0 / jnp.log(1.0 + 2.0 * jnp.maximum(plane_bound(gain, bias, channels), 1e-3))


def first_plane_kernel(
    z, head_ref, lengths_ref, gain_far, bias_far, b2_far, w1_ref, pair_ref,
    out_ref, weights_ref, normed_ref, held_ref, wide_ref, plane_ref, copies_ref, pack_ref, gain_ref, bias_ref, b2_ref,
    arrived, left_sem, sent_sem, w_sem,
):
    N, C, L, T = z.N, z.C, z.L, z.T
    cuts = (0, L // 2, L)
    parts = list(zip(cuts[:-1], cuts[1:]))
    copies = [
        pltpu.make_async_copy(pair_ref.at[pl.ds(a, b - a)], held_ref.at[pl.ds(a, b - a)], arrived.at[g]) for g, (a, b) in enumerate(parts)
    ]
    small = ((gain_far, gain_ref), (bias_far, bias_ref), (b2_far, b2_ref), (w1_ref, pack_ref.at[pl.ds(0, C)]))
    small = [pltpu.make_async_copy(there, here, w_sem.at[n]) for n, (there, here) in enumerate(small)]
    for copy in small[:1] + copies + small[1:]:
        copy.start()
    small[0].wait()
    gain = gain_ref[...]
    for copy, part in zip(copies, parts):
        copy.wait()
        for j in range(*part):
            wide_ref[:, j * C : (j + 1) * C] = normalise(held_ref[j], gain, True)
    for copy in small[1:]:
        copy.wait()
    bias = bias_ref[...].astype(f32)
    row = lax.broadcasted_iota(jnp.int32, (16, C), 0)
    pack_ref[C : C + 16] = jnp.where(row == 0, bias, b2_ref[...].astype(f32)).astype(bf16)
    first = head_ref[0] * T
    sends = [pltpu.make_async_copy(pack_ref, weights_ref, w_sem.at[4])]
    for t in range(T):
        own = wide_ref.at[:, pl.ds(pl.multiple_of((first + t) * C, 128), C)]
        sends.append(pltpu.make_async_copy(own, normed_ref.at[t], left_sem.at[t]))
    for send in sends:
        send.start()

    row = lax.broadcasted_iota(jnp.int32, (L, C), 0)
    left = jnp.concatenate([jnp.where(row == j, bias, 0.0).astype(bf16) for j in range(L)], axis=1)
    plane_ref[:, 0:N] = nt(left, wide_ref[...])
    slot = lax.broadcasted_iota(jnp.int32, (L, z.NP), 1)
    plane = jnp.where((slot < lengths_ref[0]) & (slot < N), plane_ref[...], masked_score)
    below = jnp.max(plane, axis=-1, keepdims=True) - plane
    below = jnp.where(below < 1e20, below, 0.0)
    code = jnp.round(jnp.log(1.0 + below) * log_scale(gain, bias, C)) - 32768.0
    blocks = jnp.concatenate(plane_blocks(z, code), axis=0)[0 : z.c1].astype(jnp.int32)
    copies_ref[...] = jnp.concatenate([blocks] * 4, axis=0).astype(jnp.int16)
    for n in range(z.D // 4):
        sends.append(pltpu.make_async_copy(copies_ref, out_ref.at[at(n, 4 * z.c1)], sent_sem.at[n]))
        sends[-1].start()
    for send in sends:
        send.wait()


def arranged(z, columns):
    C, W, H = z.C, z.W, z.H
    lane = lax.broadcasted_iota(jnp.int32, (C, C), 1)
    own = [column.astype(f32) for column in columns]
    parts = []
    for kind in range(4):
        moved = [own[h] if h == kind else pltpu.roll(own[h], ((h - kind) * W) % C, 1) for h in range(H)]
        alone = [jnp.where((lane >= h * W) & (lane < (h + 1) * W), moved[h], 0.0) for h in range(H)]
        parts += [sum(alone[1:], alone[0])] if kind else alone
    return jnp.concatenate([part.astype(bf16) for part in parts], axis=1)


def project(z, normed, weights, t, span, q_ref, k_ref, v_ref, g_ref):
    C, H = z.C, z.H
    projected = jnp.dot(normed, weights, preferred_element_type=f32)
    part = lambda n: projected[:, n * C : (n + 1) * C]
    for h in range(H):
        q_ref[t, h, span] = part(h).astype(bf16)
    k_ref[t, span] = part(H).astype(bf16)
    v_ref[t, span] = part(H + 1).astype(bf16)
    g_ref[t, span] = 1.0 / (1.0 + jnp.exp(-part(H + 2)))


def padding(z, t, k_ref, v_ref):
    if z.NP > z.N:
        k_ref[t, z.N :] = jnp.zeros((z.NP - z.N, z.C), bf16)
        v_ref[t, z.N :] = jnp.zeros((z.NP - z.N, z.C), bf16)


def project_kernel(z, gathered_ref, normed_ref, q_ref, k_ref, v_ref, g_ref, bias_ref, held_ref, arrived):
    C = z.C
    copy = pltpu.make_async_copy(normed_ref, held_ref, arrived.at[0])
    copy.start()
    weights = arranged(z, [gathered_ref[h, 0:C] for h in range(z.H)])
    rows = [gathered_ref[h, C : C + 16].astype(f32) for h in range(z.H)]
    bias_ref[...] = jnp.zeros_like(bias_ref)
    for h in range(z.H):
        bias_ref[h : h + 1] = rows[h][0:1]
        bias_ref[z.H + h : z.H + h + 1] = rows[h][1:2]
    copy.wait()

    def row(t):
        def block(b):
            span = at(b, z.JB)
            project(z, held_ref[t, span], weights, t, span, q_ref, k_ref, v_ref, g_ref)

        each(z.N // z.JB, block, z.small)
        padding(z, t, k_ref, v_ref)

    each(z.T, row, z.small)


def arrange_kernel(z, gathered_ref, out_ref):
    out_ref[...] = arranged(z, [gathered_ref[h] for h in range(z.H)])


def attended(z, queries, keys, values, planes):
    rows = planes[0].shape[0]
    scores = nt(queries, keys) * (log2e / math.sqrt(z.W))
    parts = []
    for h in range(z.H):
        score = scores[h * rows : (h + 1) * rows] + planes[h]
        raised = jnp.exp2(score - jnp.max(score, axis=-1, keepdims=True))
        parts.append((raised * (1.0 / jnp.sum(raised, axis=-1, keepdims=True))).astype(bf16))
    sums = jnp.dot(jnp.concatenate(parts, axis=0), values, preferred_element_type=f32)
    lane = lax.broadcasted_iota(jnp.int32, (rows, z.C), 1)
    result = sums[(z.H - 1) * rows :]
    for h in range(z.H - 2, -1, -1):
        result = jnp.where(lane < (h + 1) * z.W, sums[h * rows : (h + 1) * rows], result)
    return result


def mixed(z, t, span, q_ref, k_ref, v_ref, plane_ref):
    queries = jnp.concatenate([q_ref[t, h, span] for h in range(z.H)], axis=0)
    return attended(z, queries, k_ref[t], v_ref[t], [plane_ref[h, span] for h in range(z.H)])


def first_node_kernel(
    z, head_ref, lengths_ref, recv_ref, q_ref, k_ref, v_ref, g_ref, bias_ref, gain1_ref, out_w_ref, gain2_ref, whole_ref,
    middle_out, send_out, plane_ref, row_ref, wide_ref, own_ref, pay_ref, pair_ref, middle_ref, send_ref, arrived, sent_sem,
):
    N, T, H, D, L, C = z.N, z.T, z.H, z.D, z.L, z.C
    length = lengths_ref[0]
    copy = pltpu.make_async_copy(whole_ref.at[pl.ds(head_ref[0] * T, T)], pair_ref, arrived.at[0])
    copy.start()
    unit = 1.0 / log_scale(gain1_ref[...], bias_ref[0:H], C)
    gain2 = gain2_ref[...]
    factor_n = steps / normed_bound(gain2, C)
    blocks = up(z.p1, 8) // 8
    groups = L // 8
    seen = [lanes() + n * 128 < length for n in range(z.full)]
    seen_rest = (lanes() + z.full * 128 < length) & (lanes() < z.rest)

    def decode(r):
        chunks = recv_ref[at(r, H * z.c1)].astype(jnp.int32)
        for h in range(H):
            chunk = chunks[h * z.c1 : (h + 1) * z.c1].astype(f32)
            value = (1.0 - jnp.exp((chunk + 32768.0) * unit[h : h + 1, 0:1])) * log2e
            value = jnp.concatenate([value, value[0 : blocks * 8 - z.c1]], axis=0) if z.c1 % 8 else value
            value = [value[n * 8 : n * 8 + 8] for n in range(blocks)]
            for g in range(groups):
                target = at(r * groups + g, 8)
                for n in range(z.full):
                    plane_ref[h, target, n * 128 : n * 128 + 128] = jnp.where(seen[n], value[n * groups + g], masked_score)
                if z.rest:
                    base = z.full * groups
                    if not z.pair:
                        last = value[base + g]
                    elif g == groups - 1 and g % 2 == 0:
                        last = value[base + g // 2]
                        last = jnp.where(sublanes() < 4, last, pltpu.roll(pltpu.roll(last, 64, 1), 4, 0))
                    else:
                        last = value[base + g // 2]
                        last = pltpu.roll(last, 64, 1) if g % 2 else last
                    plane_ref[h, target, z.full * 128 :] = jnp.where(seen_rest, last, masked_score)

    each(z.R, decode, z.small)
    if not z.small:
        copy.wait()
    def row(t):
        def block(b):
            span = at(b, z.JB)
            gated = (g_ref[t, span] * mixed(z, t, span, q_ref, k_ref, v_ref, plane_ref)).astype(bf16)
            if z.small and t == 0:
                copy.wait()
            update = jnp.dot(gated, out_w_ref[...], preferred_element_type=f32)
            middle = (pair_ref[t, span].astype(f32) + update).astype(bf16)
            middle_ref[t, span] = middle
            row_ref[t, span] = normalise(middle, gain2).astype(f32)

        each(N // z.JB, block, z.small)
        for c in range(T):
            piece = row_ref[t, pl.ds(c, D, stride=T)]
            lane = t * C if isinstance(t, int) else pl.multiple_of(t * C, 128)
            wide_ref[c * D : (c + 1) * D, pl.ds(lane, C)] = piece.astype(bf16)
            pay_ref[pl.ds(z.p2 + t * T + c, D, stride=z.c2)] = jnp.round(piece * factor_n)

    each(T, row, z.small)
    sends = [pltpu.make_async_copy(middle_ref, middle_out, sent_sem.at[0])]
    sends[0].start()
    bias2 = bias_ref[H : 2 * H]
    repeated = jnp.concatenate([bias2] * T, axis=0)
    line = lax.broadcasted_iota(jnp.int32, (T * H, C), 0)
    left = jnp.concatenate([jnp.where((line >= t * H) & (line < (t + 1) * H), repeated, 0.0).astype(bf16) for t in range(T)], axis=1)
    own_ref[:, 0:N] = nt(left, wide_ref[...]) * (fine / plane_bound(gain2, repeated, C))
    high, low = digits(plane_blocks(z, own_ref[...]))
    high = jnp.concatenate(high, axis=0)[0 : z.p2]
    low = jnp.concatenate(low, axis=0)

    share = D // 4
    for n in range(4):

        @pl.loop(n * share, (n + 1) * share, unroll=4)
        def _(device):
            pay_ref[pl.ds(pl.multiple_of(device * z.c2, 8), z.p2)] = high
            pay_ref[pl.ds(pl.multiple_of(device * z.c2 + z.low2, 8), low.shape[0])] = low

        @pl.loop(n * share // 2, (n + 1) * share // 2, unroll=2)
        def _(device):
            send_ref[at(device, 2 * z.c2)] = pay_ref[at(device, 2 * z.c2)].astype(jnp.int32).astype(jnp.int16)

        span = at(n, share * z.c2)
        sends.append(pltpu.make_async_copy(send_ref.at[span], send_out.at[span], sent_sem.at[1 + n]))
        sends[-1].start()
    for send in sends:
        send.wait()


def second_node_kernel(
    z, lengths_ref, recv_ref, w_ref, bias_ref, gain2_ref, out_w_ref,
    send_ref, raw_ref, column_ref, q_ref, k_ref, v_ref, g_ref, keyed_ref, plane_ref, pay_ref,
):
    N, T, H, D, C = z.N, z.T, z.H, z.D, z.C
    length = lengths_ref[0]
    gain2 = gain2_ref[...]
    bound2 = plane_bound(gain2, bias_ref[H : 2 * H], C) * (log2e / fine)
    scale_n = normed_bound(gain2, C) * (1.0 / steps)
    blocks = up(z.p2, 8) // 8

    @pl.loop(0, D // 2, unroll=2)
    def _(pair):
        both_chunks = recv_ref[at(pair, 2 * z.c2)].astype(jnp.int32)
        for half in range(2):
            chunk = both_chunks[half * z.c2 : (half + 1) * z.c2]
            start = pl.multiple_of(pair * (2 * z.c2) + half * z.c2, 8)
            for n in range(blocks):
                high = chunk[n * 8 : n * 8 + 8]
                value = whole_value(high, chunk[z.low2 + n // 5 * 8 : z.low2 + n // 5 * 8 + 8], n)
                if (n + 1) * 8 > z.p2:
                    value = jnp.where(sublanes() < z.p2 - n * 8, value, high.astype(f32))
                raw_ref[pl.ds(start + n * 8, 8)] = value
            raw_ref[pl.ds(start + blocks * 8, z.low2 - blocks * 8)] = chunk[blocks * 8 : z.low2].astype(f32)

    def normed_rows(c):
        for t in range(T):
            piece = raw_ref[pl.ds(z.p2 + t * T + c, D, stride=z.c2)]
            column_ref[c, t * D : (t + 1) * D] = (piece * scale_n).astype(bf16)

        def inputs(b):
            span = at(b, z.JB)
            project(z, column_ref[c, span], w_ref[...], c, span, q_ref, k_ref, v_ref, g_ref)

        each(N // z.JB, inputs, z.small)
        padding(z, c, k_ref, v_ref)

    each(T, normed_rows, z.small)

    def seen(base):
        slot = lax.broadcasted_iota(jnp.int32, (1, 128), 1) + base
        return ((slot % D) * T + slot // D < length) & (slot < N)

    for h in range(H):
        for t in range(T):
            span = pl.ds(t * D, D)
            line = t * H + h
            for n in range(z.full):
                keyed_ref[h, span, n * 128 : (n + 1) * 128] = raw_ref[pl.ds(n * T * H + line, D, stride=z.c2)]
            if z.rest:
                place, turned = line, False
                if z.pair:
                    group, groups = line // 8, T * H // 8
                    if group == groups - 1 and groups % 2:
                        place, turned = group // 2 * 8 + line % 4, line % 8 >= 4
                    else:
                        place, turned = group // 2 * 8 + line % 8, group % 2 == 1
                value = raw_ref[pl.ds(z.full * T * H + place, D, stride=z.c2)]
                keyed_ref[h, span, z.full * 128 :] = pltpu.roll(value, 64, 1) if turned else value
        scale = bound2[h : h + 1, 0:1]
        for a in range(z.NP // 128):
            for b in range(z.NP // 128):
                tile = keyed_ref[h, a * 128 : (a + 1) * 128, b * 128 : (b + 1) * 128].T
                plane_ref[h, b * 128 : (b + 1) * 128, a * 128 : (a + 1) * 128] = jnp.where(seen(a * 128), tile * scale, masked_score)

    def column(c):
        def block(b):
            span = at(b, z.JB)
            gated = (g_ref[c, span] * mixed(z, c, span, q_ref, k_ref, v_ref, plane_ref)).astype(bf16)
            g_ref[c, span] = jnp.dot(gated, out_w_ref[...], preferred_element_type=f32)

        each(N // z.JB, block, z.small)
        for t in range(T):
            pay_ref[pl.ds(t * T + c, D, stride=z.c3)] = g_ref[c, t * D : (t + 1) * D]

    each(T, column, z.small)

    @pl.loop(0, D // 4, unroll=2)
    def _(device):
        send_ref[at(device, 4 * z.c3)] = pay_ref[at(device, 4 * z.c3)].astype(bf16)


def last_kernel(z, recv_ref, middle_ref, out_ref, raw_ref, row_ref):
    T, D = z.T, z.D

    @pl.loop(0, D // 4, unroll=2)
    def _(device):
        raw_ref[at(device, 4 * z.c3)] = recv_ref[at(device, 4 * z.c3)].astype(f32)

    for t in range(T):
        for c in range(T):
            row_ref[t, pl.ds(c, D, stride=T)] = raw_ref[pl.ds(t * T + c, D, stride=z.c3)]
        out_ref[t] = (middle_ref[t].astype(f32) + row_ref[t]).astype(bf16)


def call(kernel, z, shapes, scratch, scalars, operands, flops, room=6 * 2**20, far=0, out=None, hbm=False):
    near = len(operands) - scalars - far
    specs = [pl.BlockSpec(memory_space=space) for space, count in ((pltpu.SMEM, scalars), (pltpu.VMEM, near), (pltpu.HBM, far)) for _ in range(count)]
    size = lambda shape, kind: math.prod(shape) * jnp.dtype(kind).itemsize
    moved = sum(size(a.shape, a.dtype) for a in operands) + sum(size(*result) for result in shapes)
    buffers = [entry for entry in scratch if isinstance(entry, tuple)]
    held = moved + sum(size(*entry) for entry in buffers)
    return pl.pallas_call(
        functools.partial(kernel, z),
        out_shape=[(pltpu.HBM if hbm else jax.ShapeDtypeStruct)(shape, kind) for shape, kind in shapes],
        in_specs=specs,
        out_specs=[pl.BlockSpec(memory_space=out or pltpu.VMEM)] * len(shapes),
        scratch_shapes=[pltpu.VMEM(*entry) if isinstance(entry, tuple) else entry for entry in scratch],
        cost_estimate=pl.CostEstimate(flops=flops, bytes_accessed=moved, transcendentals=0),
        compiler_params=pltpu.CompilerParams(vmem_limit_bytes=min(58 * 2**20, held + room)),
        name=kernel.__name__,
    )(*operands[: scalars + near], *(pltpu.with_memory_space_constraint(a, pltpu.HBM) for a in operands[scalars + near :]))


def exchange(values, z, rows):
    C = values.shape[-1]
    shape = (z.D, rows, C) if rows % 8 == 0 else (z.D, rows // 4, 4, C)
    moved = lax.all_to_all(values.reshape(shape), both, split_axis=0, concat_axis=0, tiled=True)
    return moved.reshape(z.D * rows, C)


def shards(
    pair_tensor,
    lengths,
    starting_gain,
    starting_weights,
    starting_bias,
    starting_output,
    ending_gain,
    ending_weights,
    ending_bias,
    ending_output,
):
    H, R = lax.axis_size("heads"), lax.axis_size("rows")
    N, C = pair_tensor.shape[1:]
    z = Sizes(N, C, R, H)
    T, D, NP = z.T, z.D, z.NP
    i16 = jnp.int16
    gain1, gain2 = starting_gain.reshape(1, C), ending_gain.reshape(1, C)
    head = lax.axis_index("heads").astype(jnp.int32).reshape(1)

    dma = pltpu.SemaphoreType.DMA
    planes, packed, normed = call(
        first_plane_kernel, z,
        [((D * z.c1, C), i16), ((C + 16, C), bf16), ((T, N, C), bf16)],
        [
            ((z.L, N, C), bf16), ((N, z.L * C), bf16), ((z.L, NP), f32), ((4 * z.c1, C), i16), ((C + 16, C), bf16),
            ((1, C), f32), ((1, C), bf16), ((1, C), bf16),
            dma((z.L // 8,)), dma((T,)), dma((D // 4,)), dma((5,)),
        ],
        2, (head, lengths, gain1, starting_bias, ending_bias, starting_weights, pair_tensor),
        2 * z.L * N * C * 8, 58 * 2**20, far=5, out=pltpu.HBM, hbm=True,
    )
    planes = exchange(planes, z, z.c1)
    gathered = lax.all_gather(packed, "heads", axis=0, tiled=False)
    q, k, v, g, biases = call(
        project_kernel, z,
        [((T, H, N, C), bf16), ((T, NP, C), bf16), ((T, NP, C), bf16), ((T, N, C), f32), ((up(2 * H, 8), C), f32)],
        [((T, N, C), bf16), dma((1,))], 0, (gathered, normed), 2 * T * N * C * 7 * C, far=1,
    )
    middle, sent = call(
        first_node_kernel, z,
        [((T, N, C), bf16), ((D * z.c2, C), i16)],
        [((H, N, NP), f32), ((T, N, C), f32), ((N, T * C), bf16), ((T * H, NP), f32), ((D * z.c2, C), f32), ((T, N, C), bf16), ((T, N, C), bf16), ((D * z.c2, C), i16), dma((1,)), dma((5,))],
        2, (head, lengths, planes, q, k, v, g, biases, gain1, starting_output, gain2, pair_tensor), 4 * T * N * N * C * 2, far=1, out=pltpu.HBM, hbm=True,
    )
    received = exchange(sent, z, z.c2)
    ending_weights = lax.optimization_barrier((ending_weights, middle))[0]
    gathered = lax.all_gather(ending_weights, "heads", axis=0, tiled=False)
    (weights2,) = call(arrange_kernel, z, [((C, 7 * C), bf16)], [], 0, (gathered,), 4 * C * C)
    (sent,) = call(
        second_node_kernel, z,
        [((D * z.c3, C), bf16)],
        [
            ((D * z.c2, C), f32), ((T, N, C), bf16), ((T, H, N, C), bf16), ((T, NP, C), bf16), ((T, NP, C), bf16), ((T, N, C), f32),
            ((H, NP, NP), f32), ((H, NP, NP), f32), ((D * z.c3, C), f32),
        ],
        1, (lengths, received, weights2, biases, gain2, ending_output), 4 * T * N * N * C * 2,
    )
    received = exchange(sent, z, z.c3)
    (refined,) = call(
        last_kernel, z, [((T, N, C), bf16)], [((D * z.c3, C), f32), ((T, N, C), f32)], 0, (received, middle), T * N * C
    )
    return refined


def solution(mesh):
    placed = (
        P("rows", None, None),
        P(),
        P(),
        P(None, "heads"),
        P("heads", None),
        P(),
        P(),
        P(None, "heads"),
        P("heads", None),
        P(),
    )
    return jax.shard_map(
        shards,
        mesh=mesh,
        in_specs=placed,
        out_specs=P(both, None, None),
        check_vma=False,
    )
```

```python
import functools
import math

import jax
import jax.numpy as jnp
from jax import lax
from jax.experimental import pallas as pl
from jax.experimental.pallas import tpu as pltpu
from jax.sharding import PartitionSpec as P

epsilon = 1e-05
masked_score = -1e30
log2e = math.log2(math.e)
steps = 32767.0
fine = 262143.0
f32 = jnp.float32
bf16 = jnp.bfloat16
both = ("rows", "heads")


def up(value, multiple):
    return -(-value // multiple) * multiple


class Sizes:
    def __init__(self, tokens, channels, row_devices, heads):
        self.N, self.C, self.R, self.H = tokens, channels, row_devices, heads
        self.D = row_devices * heads
        self.L = tokens // row_devices
        self.T = tokens // self.D
        self.NP = up(tokens, 128)
        self.W = channels // heads
        self.full = tokens // 128
        self.rest = tokens % 128
        self.pair = self.rest == 64
        self.p1, self.c1 = self.planes(self.L)
        self.c1 = up(self.p1, 4)
        self.p2, self.c2 = self.planes(self.T * heads)
        self.low2 = up(self.p2 + self.T * self.T, 8)
        self.c2 = up(self.low2 + self.c2, 8)
        self.c3 = up(self.T * self.T, 4)
        self.small = tokens <= 256
        self.JB = tokens if self.small else 192

    def planes(self, rows):
        groups = rows // 8
        count = rows * self.full
        if self.pair:
            count += 8 * (groups // 2) + 4 * (groups % 2)
        elif self.rest:
            count += rows
        return count, 8 * (-(-(-(-count // 8)) // 5))


def each(count, body, unrolled=False):
    if count == 1 or unrolled:
        for index in range(count):
            body(index)
    else:

        @pl.loop(0, count)
        def _(index):
            body(index)


def at(index, size):
    if isinstance(index, int):
        return pl.ds(index * size, size)
    return pl.ds(pl.multiple_of(index * size, 8), size)


def nt(left, right):
    return lax.dot_general(left, right, (((1,), (1,)), ((), ())), preferred_element_type=f32)


def normalise(values, gain, multiplied=False):
    C = values.shape[-1]
    widened = values.astype(f32)
    if multiplied and C & (C - 1) == 0:
        centre = jnp.dot(values, jnp.full((C, C), 1.0 / C, bf16), preferred_element_type=f32)
    else:
        centre = jnp.mean(widened, axis=-1, keepdims=True)
    shifted = widened - centre
    spread = jnp.mean(shifted * shifted, axis=-1, keepdims=True)
    return (shifted * lax.rsqrt(spread + epsilon) * gain).astype(bf16)


def plane_bound(gain, bias, channels):
    product = gain * bias
    norm = jnp.sqrt(jnp.sum(product * product, axis=-1, keepdims=True))
    return jnp.maximum(norm * (1.01 * math.sqrt(channels)), 1e-6)


def normed_bound(gain, channels):
    return jnp.max(jnp.abs(gain), axis=-1, keepdims=True) * (1.01 * math.sqrt(channels))


def lanes(rows=8):
    return lax.broadcasted_iota(jnp.int32, (rows, 128), 1)


def sublanes():
    return lax.broadcasted_iota(jnp.int32, (8, 128), 0)


def plane_blocks(z, values):
    groups = values.shape[0] // 8
    blocks = [values[g * 8 : g * 8 + 8, n * 128 : n * 128 + 128] for n in range(z.full) for g in range(groups)]
    if z.rest:
        last = [values[g * 8 : g * 8 + 8, z.full * 128 :] for g in range(groups)]
        if z.pair:
            for g in range(0, groups - 1, 2):
                blocks.append(jnp.where(lanes() < 64, last[g], pltpu.roll(last[g + 1], 64, 1)))
            if groups % 2:
                blocks.append(jnp.where(lanes() < 64, last[-1], pltpu.roll(pltpu.roll(last[-1], 64, 1), 4, 0)))
        else:
            blocks += last
    return blocks


def digits(blocks):
    high, low = [], []
    for n, block in enumerate(blocks):
        whole = jnp.round(block).astype(jnp.int32)
        upper = (whole + 4) >> 3
        digit = (whole - upper * 8 + 4) << (3 * (n % 5))
        high.append(upper.astype(f32))
        low = low + [digit] if n % 5 == 0 else low[:-1] + [low[-1] + digit]
    return high, [block.astype(f32) for block in low]


def whole_value(high, low, number):
    return (high * 8 + ((low >> (3 * (number % 5))) & 7) - 4).astype(f32)


def log_scale(gain, bias, channels):
    return 65535.0 / jnp.log(1.0 + 2.0 * jnp.maximum(plane_bound(gain, bias, channels), 1e-3))


def first_plane_kernel(
    z, head_ref, lengths_ref, gain_far, bias_far, b2_far, w1_ref, pair_ref,
    out_ref, weights_ref, normed_ref, held_ref, wide_ref, plane_ref, copies_ref, pack_ref, gain_ref, bias_ref, b2_ref,
    arrived, left_sem, sent_sem, w_sem,
):
    N, C, L, T = z.N, z.C, z.L, z.T
    cuts = (0, L // 2, L)
    parts = list(zip(cuts[:-1], cuts[1:]))
    copies = [
        pltpu.make_async_copy(pair_ref.at[pl.ds(a, b - a)], held_ref.at[pl.ds(a, b - a)], arrived.at[g]) for g, (a, b) in enumerate(parts)
    ]
    small = ((gain_far, gain_ref), (bias_far, bias_ref), (b2_far, b2_ref), (w1_ref, pack_ref.at[pl.ds(0, C)]))
    small = [pltpu.make_async_copy(there, here, w_sem.at[n]) for n, (there, here) in enumerate(small)]
    for copy in small[:1] + copies + small[1:]:
        copy.start()
    small[0].wait()
    gain = gain_ref[...]
    for copy, part in zip(copies, parts):
        copy.wait()
        for j in range(*part):
            wide_ref[:, j * C : (j + 1) * C] = normalise(held_ref[j], gain, True)
    for copy in small[1:]:
        copy.wait()
    bias = bias_ref[...].astype(f32)
    row = lax.broadcasted_iota(jnp.int32, (16, C), 0)
    pack_ref[C : C + 16] = jnp.where(row == 0, bias, b2_ref[...].astype(f32)).astype(bf16)
    first = head_ref[0] * T
    sends = [pltpu.make_async_copy(pack_ref, weights_ref, w_sem.at[4])]
    for t in range(T):
        own = wide_ref.at[:, pl.ds(pl.multiple_of((first + t) * C, 128), C)]
        sends.append(pltpu.make_async_copy(own, normed_ref.at[t], left_sem.at[t]))
    for send in sends:
        send.start()

    row = lax.broadcasted_iota(jnp.int32, (L, C), 0)
    left = jnp.concatenate([jnp.where(row == j, bias, 0.0).astype(bf16) for j in range(L)], axis=1)
    plane_ref[:, 0:N] = nt(left, wide_ref[...])
    slot = lax.broadcasted_iota(jnp.int32, (L, z.NP), 1)
    plane = jnp.where((slot < lengths_ref[0]) & (slot < N), plane_ref[...], masked_score)
    below = jnp.max(plane, axis=-1, keepdims=True) - plane
    below = jnp.where(below < 1e20, below, 0.0)
    code = jnp.round(jnp.log(1.0 + below) * log_scale(gain, bias, C)) - 32768.0
    blocks = jnp.concatenate(plane_blocks(z, code), axis=0)[0 : z.c1].astype(jnp.int32)
    copies_ref[...] = jnp.concatenate([blocks] * 4, axis=0).astype(jnp.int16)
    for n in range(z.D // 4):
        sends.append(pltpu.make_async_copy(copies_ref, out_ref.at[at(n, 4 * z.c1)], sent_sem.at[n]))
        sends[-1].start()
    for send in sends:
        send.wait()


def arranged(z, columns):
    C, W, H = z.C, z.W, z.H
    lane = lax.broadcasted_iota(jnp.int32, (C, C), 1)
    own = [column.astype(f32) for column in columns]
    parts = []
    for kind in range(4):
        moved = [own[h] if h == kind else pltpu.roll(own[h], ((h - kind) * W) % C, 1) for h in range(H)]
        alone = [jnp.where((lane >= h * W) & (lane < (h + 1) * W), moved[h], 0.0) for h in range(H)]
        parts += [sum(alone[1:], alone[0])] if kind else alone
    return jnp.concatenate([part.astype(bf16) for part in parts], axis=1)


def project(z, normed, weights, t, span, q_ref, k_ref, v_ref, g_ref):
    C, H = z.C, z.H
    projected = jnp.dot(normed, weights, preferred_element_type=f32)
    part = lambda n: projected[:, n * C : (n + 1) * C]
    for h in range(H):
        q_ref[t, h, span] = part(h).astype(bf16)
    k_ref[t, span] = part(H).astype(bf16)
    v_ref[t, span] = part(H + 1).astype(bf16)
    g_ref[t, span] = 1.0 / (1.0 + jnp.exp(-part(H + 2)))


def padding(z, t, k_ref, v_ref):
    if z.NP > z.N:
        k_ref[t, z.N :] = jnp.zeros((z.NP - z.N, z.C), bf16)
        v_ref[t, z.N :] = jnp.zeros((z.NP - z.N, z.C), bf16)


def project_kernel(z, gathered_ref, normed_ref, q_ref, k_ref, v_ref, g_ref, bias_ref, held_ref, arrived):
    C = z.C
    copy = pltpu.make_async_copy(normed_ref, held_ref, arrived.at[0])
    copy.start()
    weights = arranged(z, [gathered_ref[h, 0:C] for h in range(z.H)])
    rows = [gathered_ref[h, C : C + 16].astype(f32) for h in range(z.H)]
    bias_ref[...] = jnp.zeros_like(bias_ref)
    for h in range(z.H):
        bias_ref[h : h + 1] = rows[h][0:1]
        bias_ref[z.H + h : z.H + h + 1] = rows[h][1:2]
    copy.wait()

    def row(t):
        def block(b):
            span = at(b, z.JB)
            project(z, held_ref[t, span], weights, t, span, q_ref, k_ref, v_ref, g_ref)

        each(z.N // z.JB, block, z.small)
        padding(z, t, k_ref, v_ref)

    each(z.T, row, z.small)


def arrange_kernel(z, gathered_ref, out_ref):
    out_ref[...] = arranged(z, [gathered_ref[h] for h in range(z.H)])


def attended(z, queries, keys, values, planes):
    rows = planes[0].shape[0]
    scores = nt(queries, keys) * (log2e / math.sqrt(z.W))
    parts = []
    for h in range(z.H):
        score = scores[h * rows : (h + 1) * rows] + planes[h]
        raised = jnp.exp2(score - jnp.max(score, axis=-1, keepdims=True))
        parts.append((raised * (1.0 / jnp.sum(raised, axis=-1, keepdims=True))).astype(bf16))
    sums = jnp.dot(jnp.concatenate(parts, axis=0), values, preferred_element_type=f32)
    lane = lax.broadcasted_iota(jnp.int32, (rows, z.C), 1)
    result = sums[(z.H - 1) * rows :]
    for h in range(z.H - 2, -1, -1):
        result = jnp.where(lane < (h + 1) * z.W, sums[h * rows : (h + 1) * rows], result)
    return result


def mixed(z, t, span, q_ref, k_ref, v_ref, plane_ref):
    queries = jnp.concatenate([q_ref[t, h, span] for h in range(z.H)], axis=0)
    return attended(z, queries, k_ref[t], v_ref[t], [plane_ref[h, span] for h in range(z.H)])


def first_node_kernel(
    z, head_ref, lengths_ref, recv_ref, q_ref, k_ref, v_ref, g_ref, bias_ref, gain1_ref, out_w_ref, gain2_ref, whole_ref,
    middle_out, send_out, plane_ref, row_ref, wide_ref, own_ref, pay_ref, pair_ref, middle_ref, send_ref, arrived, sent_sem,
):
    N, T, H, D, L, C = z.N, z.T, z.H, z.D, z.L, z.C
    length = lengths_ref[0]
    copy = pltpu.make_async_copy(whole_ref.at[pl.ds(head_ref[0] * T, T)], pair_ref, arrived.at[0])
    copy.start()
    unit = 1.0 / log_scale(gain1_ref[...], bias_ref[0:H], C)
    gain2 = gain2_ref[...]
    factor_n = steps / normed_bound(gain2, C)
    blocks = up(z.p1, 8) // 8
    groups = L // 8
    seen = [lanes() + n * 128 < length for n in range(z.full)]
    seen_rest = (lanes() + z.full * 128 < length) & (lanes() < z.rest)

    def decode(r):
        chunks = recv_ref[at(r, H * z.c1)].astype(jnp.int32)
        for h in range(H):
            chunk = chunks[h * z.c1 : (h + 1) * z.c1].astype(f32)
            value = (1.0 - jnp.exp((chunk + 32768.0) * unit[h : h + 1, 0:1])) * log2e
            value = jnp.concatenate([value, value[0 : blocks * 8 - z.c1]], axis=0) if z.c1 % 8 else value
            value = [value[n * 8 : n * 8 + 8] for n in range(blocks)]
            for g in range(groups):
                target = at(r * groups + g, 8)
                for n in range(z.full):
                    plane_ref[h, target, n * 128 : n * 128 + 128] = jnp.where(seen[n], value[n * groups + g], masked_score)
                if z.rest:
                    base = z.full * groups
                    if not z.pair:
                        last = value[base + g]
                    elif g == groups - 1 and g % 2 == 0:
                        last = value[base + g // 2]
                        last = jnp.where(sublanes() < 4, last, pltpu.roll(pltpu.roll(last, 64, 1), 4, 0))
                    else:
                        last = value[base + g // 2]
                        last = pltpu.roll(last, 64, 1) if g % 2 else last
                    plane_ref[h, target, z.full * 128 :] = jnp.where(seen_rest, last, masked_score)

    each(z.R, decode, z.small)
    if not z.small:
        copy.wait()
    def row(t):
        def block(b):
            span = at(b, z.JB)
            gated = (g_ref[t, span] * mixed(z, t, span, q_ref, k_ref, v_ref, plane_ref)).astype(bf16)
            if z.small and t == 0:
                copy.wait()
            update = jnp.dot(gated, out_w_ref[...], preferred_element_type=f32)
            middle = (pair_ref[t, span].astype(f32) + update).astype(bf16)
            middle_ref[t, span] = middle
            row_ref[t, span] = normalise(middle, gain2).astype(f32)

        each(N // z.JB, block, z.small)
        for c in range(T):
            piece = row_ref[t, pl.ds(c, D, stride=T)]
            lane = t * C if isinstance(t, int) else pl.multiple_of(t * C, 128)
            wide_ref[c * D : (c + 1) * D, pl.ds(lane, C)] = piece.astype(bf16)
            pay_ref[pl.ds(z.p2 + t * T + c, D, stride=z.c2)] = jnp.round(piece * factor_n)

    each(T, row, z.small)
    sends = [pltpu.make_async_copy(middle_ref, middle_out, sent_sem.at[0])]
    sends[0].start()
    bias2 = bias_ref[H : 2 * H]
    repeated = jnp.concatenate([bias2] * T, axis=0)
    line = lax.broadcasted_iota(jnp.int32, (T * H, C), 0)
    left = jnp.concatenate([jnp.where((line >= t * H) & (line < (t + 1) * H), repeated, 0.0).astype(bf16) for t in range(T)], axis=1)
    own_ref[:, 0:N] = nt(left, wide_ref[...]) * (fine / plane_bound(gain2, repeated, C))
    high, low = digits(plane_blocks(z, own_ref[...]))
    high = jnp.concatenate(high, axis=0)[0 : z.p2]
    low = jnp.concatenate(low, axis=0)

    share = D // 4
    for n in range(4):

        @pl.loop(n * share, (n + 1) * share, unroll=4)
        def _(device):
            pay_ref[pl.ds(pl.multiple_of(device * z.c2, 8), z.p2)] = high
            pay_ref[pl.ds(pl.multiple_of(device * z.c2 + z.low2, 8), low.shape[0])] = low

        @pl.loop(n * share // 2, (n + 1) * share // 2, unroll=2)
        def _(device):
            send_ref[at(device, 2 * z.c2)] = pay_ref[at(device, 2 * z.c2)].astype(jnp.int32).astype(jnp.int16)

        span = at(n, share * z.c2)
        sends.append(pltpu.make_async_copy(send_ref.at[span], send_out.at[span], sent_sem.at[1 + n]))
        sends[-1].start()
    for send in sends:
        send.wait()


def second_node_kernel(
    z, lengths_ref, recv_ref, w_ref, bias_ref, gain2_ref, out_w_ref,
    send_ref, raw_ref, column_ref, q_ref, k_ref, v_ref, g_ref, keyed_ref, plane_ref, pay_ref,
):
    N, T, H, D, C = z.N, z.T, z.H, z.D, z.C
    length = lengths_ref[0]
    gain2 = gain2_ref[...]
    bound2 = plane_bound(gain2, bias_ref[H : 2 * H], C) * (log2e / fine)
    scale_n = normed_bound(gain2, C) * (1.0 / steps)
    blocks = up(z.p2, 8) // 8

    @pl.loop(0, D // 2, unroll=2)
    def _(pair):
        both_chunks = recv_ref[at(pair, 2 * z.c2)].astype(jnp.int32)
        for half in range(2):
            chunk = both_chunks[half * z.c2 : (half + 1) * z.c2]
            start = pl.multiple_of(pair * (2 * z.c2) + half * z.c2, 8)
            for n in range(blocks):
                high = chunk[n * 8 : n * 8 + 8]
                value = whole_value(high, chunk[z.low2 + n // 5 * 8 : z.low2 + n // 5 * 8 + 8], n)
                if (n + 1) * 8 > z.p2:
                    value = jnp.where(sublanes() < z.p2 - n * 8, value, high.astype(f32))
                raw_ref[pl.ds(start + n * 8, 8)] = value
            raw_ref[pl.ds(start + blocks * 8, z.low2 - blocks * 8)] = chunk[blocks * 8 : z.low2].astype(f32)

    def normed_rows(c):
        for t in range(T):
            piece = raw_ref[pl.ds(z.p2 + t * T + c, D, stride=z.c2)]
            column_ref[c, t * D : (t + 1) * D] = (piece * scale_n).astype(bf16)

        def inputs(b):
            span = at(b, z.JB)
            project(z, column_ref[c, span], w_ref[...], c, span, q_ref, k_ref, v_ref, g_ref)

        each(N // z.JB, inputs, z.small)
        padding(z, c, k_ref, v_ref)

    each(T, normed_rows, z.small)

    def seen(base):
        slot = lax.broadcasted_iota(jnp.int32, (1, 128), 1) + base
        return ((slot % D) * T + slot // D < length) & (slot < N)

    for h in range(H):
        for t in range(T):
            span = pl.ds(t * D, D)
            line = t * H + h
            for n in range(z.full):
                keyed_ref[h, span, n * 128 : (n + 1) * 128] = raw_ref[pl.ds(n * T * H + line, D, stride=z.c2)]
            if z.rest:
                place, turned = line, False
                if z.pair:
                    group, groups = line // 8, T * H // 8
                    if group == groups - 1 and groups % 2:
                        place, turned = group // 2 * 8 + line % 4, line % 8 >= 4
                    else:
                        place, turned = group // 2 * 8 + line % 8, group % 2 == 1
                value = raw_ref[pl.ds(z.full * T * H + place, D, stride=z.c2)]
                keyed_ref[h, span, z.full * 128 :] = pltpu.roll(value, 64, 1) if turned else value
        scale = bound2[h : h + 1, 0:1]
        for a in range(z.NP // 128):
            for b in range(z.NP // 128):
                tile = keyed_ref[h, a * 128 : (a + 1) * 128, b * 128 : (b + 1) * 128].T
                plane_ref[h, b * 128 : (b + 1) * 128, a * 128 : (a + 1) * 128] = jnp.where(seen(a * 128), tile * scale, masked_score)

    def column(c):
        def block(b):
            span = at(b, z.JB)
            gated = (g_ref[c, span] * mixed(z, c, span, q_ref, k_ref, v_ref, plane_ref)).astype(bf16)
            g_ref[c, span] = jnp.dot(gated, out_w_ref[...], preferred_element_type=f32)

        each(N // z.JB, block, z.small)
        for t in range(T):
            pay_ref[pl.ds(t * T + c, D, stride=z.c3)] = g_ref[c, t * D : (t + 1) * D]

    each(T, column, z.small)

    @pl.loop(0, D // 4, unroll=2)
    def _(device):
        send_ref[at(device, 4 * z.c3)] = pay_ref[at(device, 4 * z.c3)].astype(bf16)


def last_kernel(z, recv_ref, middle_ref, out_ref, raw_ref, row_ref):
    T, D = z.T, z.D

    @pl.loop(0, D // 4, unroll=2)
    def _(device):
        raw_ref[at(device, 4 * z.c3)] = recv_ref[at(device, 4 * z.c3)].astype(f32)

    for t in range(T):
        for c in range(T):
            row_ref[t, pl.ds(c, D, stride=T)] = raw_ref[pl.ds(t * T + c, D, stride=z.c3)]
        out_ref[t] = (middle_ref[t].astype(f32) + row_ref[t]).astype(bf16)


def call(kernel, z, shapes, scratch, scalars, operands, flops, room=6 * 2**20, far=0, out=None, hbm=False):
    near = len(operands) - scalars - far
    specs = [pl.BlockSpec(memory_space=space) for space, count in ((pltpu.SMEM, scalars), (pltpu.VMEM, near), (pltpu.HBM, far)) for _ in range(count)]
    size = lambda shape, kind: math.prod(shape) * jnp.dtype(kind).itemsize
    moved = sum(size(a.shape, a.dtype) for a in operands) + sum(size(*result) for result in shapes)
    buffers = [entry for entry in scratch if isinstance(entry, tuple)]
    held = moved + sum(size(*entry) for entry in buffers)
    return pl.pallas_call(
        functools.partial(kernel, z),
        out_shape=[(pltpu.HBM if hbm else jax.ShapeDtypeStruct)(shape, kind) for shape, kind in shapes],
        in_specs=specs,
        out_specs=[pl.BlockSpec(memory_space=out or pltpu.VMEM)] * len(shapes),
        scratch_shapes=[pltpu.VMEM(*entry) if isinstance(entry, tuple) else entry for entry in scratch],
        cost_estimate=pl.CostEstimate(flops=flops, bytes_accessed=moved, transcendentals=0),
        compiler_params=pltpu.CompilerParams(vmem_limit_bytes=min(58 * 2**20, held + room)),
        name=kernel.__name__,
    )(*operands[: scalars + near], *(pltpu.with_memory_space_constraint(a, pltpu.HBM) for a in operands[scalars + near :]))


def exchange(values, z, rows):
    C = values.shape[-1]
    shape = (z.D, rows, C) if rows % 8 == 0 else (z.D, rows // 4, 4, C)
    moved = lax.all_to_all(values.reshape(shape), both, split_axis=0, concat_axis=0, tiled=True)
    return moved.reshape(z.D * rows, C)


def shards(
    pair_tensor,
    lengths,
    starting_gain,
    starting_weights,
    starting_bias,
    starting_output,
    ending_gain,
    ending_weights,
    ending_bias,
    ending_output,
):
    H, R = lax.axis_size("heads"), lax.axis_size("rows")
    N, C = pair_tensor.shape[1:]
    z = Sizes(N, C, R, H)
    T, D, NP = z.T, z.D, z.NP
    i16 = jnp.int16
    gain1, gain2 = starting_gain.reshape(1, C), ending_gain.reshape(1, C)
    head = lax.axis_index("heads").astype(jnp.int32).reshape(1)

    dma = pltpu.SemaphoreType.DMA
    planes, packed, normed = call(
        first_plane_kernel, z,
        [((D * z.c1, C), i16), ((C + 16, C), bf16), ((T, N, C), bf16)],
        [
            ((z.L, N, C), bf16), ((N, z.L * C), bf16), ((z.L, NP), f32), ((4 * z.c1, C), i16), ((C + 16, C), bf16),
            ((1, C), f32), ((1, C), bf16), ((1, C), bf16),
            dma((z.L // 8,)), dma((T,)), dma((D // 4,)), dma((5,)),
        ],
        2, (head, lengths, gain1, starting_bias, ending_bias, starting_weights, pair_tensor),
        2 * z.L * N * C * 8, 58 * 2**20, far=5, out=pltpu.HBM, hbm=True,
    )
    planes = exchange(planes, z, z.c1)
    gathered = lax.all_gather(packed, "heads", axis=0, tiled=False)
    q, k, v, g, biases = call(
        project_kernel, z,
        [((T, H, N, C), bf16), ((T, NP, C), bf16), ((T, NP, C), bf16), ((T, N, C), f32), ((up(2 * H, 8), C), f32)],
        [((T, N, C), bf16), dma((1,))], 0, (gathered, normed), 2 * T * N * C * 7 * C, far=1,
    )
    middle, sent = call(
        first_node_kernel, z,
        [((T, N, C), bf16), ((D * z.c2, C), i16)],
        [((H, N, NP), f32), ((T, N, C), f32), ((N, T * C), bf16), ((T * H, NP), f32), ((D * z.c2, C), f32), ((T, N, C), bf16), ((T, N, C), bf16), ((D * z.c2, C), i16), dma((1,)), dma((5,))],
        2, (head, lengths, planes, q, k, v, g, biases, gain1, starting_output, gain2, pair_tensor), 4 * T * N * N * C * 2, far=1, out=pltpu.HBM, hbm=True,
    )
    received = exchange(sent, z, z.c2)
    ending_weights = lax.optimization_barrier((ending_weights, middle))[0]
    gathered = lax.all_gather(ending_weights, "heads", axis=0, tiled=False)
    (weights2,) = call(arrange_kernel, z, [((C, 7 * C), bf16)], [], 0, (gathered,), 4 * C * C)
    (sent,) = call(
        second_node_kernel, z,
        [((D * z.c3, C), bf16)],
        [
            ((D * z.c2, C), f32), ((T, N, C), bf16), ((T, H, N, C), bf16), ((T, NP, C), bf16), ((T, NP, C), bf16), ((T, N, C), f32),
            ((H, NP, NP), f32), ((H, NP, NP), f32), ((D * z.c3, C), f32),
        ],
        1, (lengths, received, weights2, biases, gain2, ending_output), 4 * T * N * N * C * 2,
    )
    received = exchange(sent, z, z.c3)
    (refined,) = call(
        last_kernel, z, [((T, N, C), bf16)], [((D * z.c3, C), f32), ((T, N, C), f32)], 0, (received, middle), T * N * C
    )
    return refined


def solution(mesh):
    placed = (
        P("rows", None, None),
        P(),
        P(),
        P(None, "heads"),
        P("heads", None),
        P(),
        P(),
        P(None, "heads"),
        P("heads", None),
        P(),
    )
    return jax.shard_map(
        shards,
        mesh=mesh,
        in_specs=placed,
        out_specs=P(both, None, None),
        check_vma=False,
    )
```
